128 devices in a mesh: dp: 16 (over x_hi, z, core), mp: 8 (over y, x_lo).
Axes of the slice: x: 4 (x_hi: 2, x_lo: 2; x = x_hi * 2 + x_lo), y: 4, z: 4, core: 2. Of those that a mesh axis runs over, the one named last changes fastest.
Arguments:
- events: bfloat16 [4096, 128, 8, 128], P('dp', 'mp'), may hold values from -32 to 32
- lengths: int32 [4096, 128], P('dp', 'mp'), may hold values from 2 to 8, as said below
- query_vecs: bfloat16 [128, 128], P('mp'), may hold values from -5 to 5
- fm_proj: bfloat16 [128, 8], replicated, may hold values from -0.5 to 0.5
- up_weight: bfloat16 [1024, 16384], P(None, 'mp'), may hold values from -0.1875 to 0.1875
- down_weight: bfloat16 [16384, 512], P('mp'), may hold values from -0.046875 to 0.046875
- cotangent: bfloat16 [4096, 512], P('dp', 'mp'), may hold values from -1.5 to 1.5
Outputs:
- block_out: bfloat16 [4096, 512], P('dp', 'mp')
- grad_up: float32 [1024, 16384], P(None, 'mp')
- grad_down: float32 [16384, 512], P('mp')
- grad_pooled: bfloat16 [4096, 128, 128], P('dp', 'mp')
- grad_query: float32 [128, 128], P('mp')
The draws below stay inside these ranges and needn't reach their ends.
Inputs may be any that keep to these rules, and one draw needn't show every extreme that they name: `lengths`: every length of the first user equals 8.
All inputs are finite; a program needn't handle non-finite values.
Results may differ from the reference program's by a relative error of at most 0.024.
Values may be sent and summed in bfloat16 or wider, within the bound.
No kernel may reach another device: no remote copies, remote signals or barrier semaphores. Data moves between devices by JAX's collectives and lax.ppermute only.
A program may use at most 128 MiB of HBM per device.

```python
import math
import jax
import jax.numpy as jnp
from jax import lax

E = 128
F = 128
L = 8
RANK = 8
HID = 16384
OUT = 512
B_DEV = 256
K = 1024
USERS = 4096
N_DP = 16


def shared_draw(key):
    query_key = jax.random.fold_in(key, 11)
    event_key = jax.random.fold_in(key, 12)
    query_vecs = jnp.clip(jax.random.normal(query_key, (F, E), jnp.float32), -5.0, 5.0)
    events = jax.random.normal(event_key, (USERS, F, L, E), jnp.float32)
    return (events, query_vecs)


def draw_events(key, part):
    events, query_vecs = shared_draw(key)
    return events.astype(jnp.bfloat16)


def draw_query_vecs(key, part):
    events, query_vecs = shared_draw(key)
    return query_vecs.astype(jnp.bfloat16)


def draw_lengths(key, part):
    heavy_key = jax.random.fold_in(key, 21)
    length_key = jax.random.fold_in(key, 22)
    heaviness = jax.random.randint(heavy_key, (USERS, 1), 0, 3)
    ceiling = L // 4 * jnp.where(heaviness == 0, 1, jnp.where(heaviness == 1, 2, 4))
    lengths = jax.random.randint(length_key, (USERS, F), 2, ceiling + 1)
    lengths = lengths.at[0, :].set(L)
    lengths = lengths.at[1, 0].set(2)
    return lengths.astype(jnp.int32)


def block_levels(key, shape, shards, low, high):
    factor_of, own = 1.0, jax.random.fold_in(key, 6)
    for position, shards_of in shards:
        draws = jnp.exp(jax.random.uniform(jax.random.fold_in(own, position), (shards_of,), jnp.float32, low / len(shards), high / len(shards)))
        factor_of = factor_of * jnp.repeat(draws, shape[position] // shards_of).reshape([-1 if axis == position else 1 for axis in range(len(shape))])
    return factor_of


def bell_draw(key, shape, spread, most, split=(), kind=jnp.bfloat16):
    values = spread * jax.random.normal(key, shape, jnp.float32)
    if split:
        values = values * block_levels(key, shape, split, -0.22, 0.18)
    return jnp.clip(values, -most, most).astype(kind)


def setup_inputs(seed: int = 0) -> dict:
    key_list = jax.random.split(jax.random.key(seed), 8)
    events = draw_events(jax.random.fold_in(key_list[7], 71), 0)
    lengths = draw_lengths(jax.random.fold_in(key_list[7], 71), 0)
    query_vecs = draw_query_vecs(jax.random.fold_in(key_list[7], 71), 0)
    fm_proj = bell_draw(key_list[3], (F, RANK), F ** -0.5, 0.5)
    up_weight = bell_draw(key_list[4], (K, HID), K ** -0.5, 0.1875, ((1, 8),))
    down_weight = bell_draw(key_list[5], (HID, OUT), HID ** -0.5, 0.046875, ((0, 8),))
    cotangent = bell_draw(key_list[6], (USERS, OUT), 0.25, 1.5, ((0, 16), (1, 8)))
    return {"events": events, "lengths": lengths, "query_vecs": query_vecs, "fm_proj": fm_proj, "up_weight": up_weight, "down_weight": down_weight, "cotangent": cotangent}


norm_eps = 1e-05
highest = lax.Precision.HIGHEST

def pool_shard(ev_block, len_block, query_f32, score_scale):
    ev_f32 = ev_block.astype(jnp.float32)
    scores = jnp.einsum('bfle,fe->bfl', ev_f32, query_f32, precision=highest) * score_scale
    positions = jnp.arange(ev_block.shape[2]).astype(jnp.int32)
    live_mask = positions[None, None, :] < len_block[:, :, None]
    row_top = lax.optimization_barrier(jnp.max(jnp.where(live_mask, scores, -1e+30), axis=-1, keepdims=True))
    exp_scores = jnp.exp(jnp.where(live_mask, scores - row_top, -1e+30))
    weights = exp_scores / lax.optimization_barrier(jnp.sum(exp_scores, axis=-1, keepdims=True))
    rounded = lax.optimization_barrier(weights.astype(jnp.bfloat16)).astype(jnp.float32)
    pooled = jnp.einsum('bfl,bfle->bfe', rounded, ev_f32, precision=highest).astype(jnp.bfloat16)
    return (pooled, weights)

def query_shard(pieces, score_scale):
    ev_block, weights, grad_rows = pieces
    ev_f32 = ev_block.astype(jnp.float32)
    contrib = jnp.einsum('bfle,bfe->bfl', ev_f32, grad_rows.astype(jnp.float32), precision=highest)
    d_scores = weights * (contrib - lax.optimization_barrier(jnp.sum(weights * contrib, axis=-1, keepdims=True)))
    d_scores = lax.optimization_barrier(d_scores.astype(jnp.bfloat16)).astype(jnp.float32)
    query_term = jnp.einsum('bfl,bfle->fe', d_scores, ev_f32, precision=highest) * score_scale
    return lax.optimization_barrier(query_term.astype(jnp.bfloat16)).astype(jnp.float32)

def reference(events, lengths, query_vecs, fm_proj, up_weight, down_weight, cotangent):
    user_count = events.shape[0]
    score_scale = 1.0 / math.sqrt(E)
    query_f32 = query_vecs.astype(jnp.float32)
    ev_blocks = events.reshape(N_DP, B_DEV, F, L, E)
    len_blocks = lengths.reshape(N_DP, B_DEV, F)
    pooled, weights = lax.map(lambda pieces: pool_shard(pieces[0], pieces[1], query_f32, score_scale), (ev_blocks, len_blocks))
    pooled = pooled.reshape(user_count, F, E)
    pooled_f32 = pooled.astype(jnp.float32)
    proj_f32 = fm_proj.astype(jnp.float32)
    proj_mix = jnp.einsum('bfe,fr->bre', pooled_f32, proj_f32, precision=highest).astype(jnp.bfloat16)
    mix_f32 = proj_mix.astype(jnp.float32)
    fm_full = jnp.einsum('bfe,bre->bfr', pooled_f32, mix_f32, precision=highest).reshape(user_count, F * RANK)
    inv_rms = lax.rsqrt(lax.optimization_barrier(jnp.mean(fm_full * fm_full, axis=-1, keepdims=True)) + norm_eps)
    normed = fm_full * inv_rms
    normed_b = normed.astype(jnp.bfloat16)
    hidden = jnp.dot(normed_b, up_weight, preferred_element_type=jnp.float32)
    activated = jax.nn.silu(hidden).astype(jnp.bfloat16)
    block_out = jnp.dot(activated, down_weight, preferred_element_type=jnp.float32).astype(jnp.bfloat16)
    d_act = jnp.dot(cotangent, down_weight.T, preferred_element_type=jnp.float32)
    sig_hidden = jax.nn.sigmoid(hidden)
    d_hidden = (d_act * sig_hidden * (1.0 + hidden * (1.0 - sig_hidden))).astype(jnp.bfloat16)

    def add_shard(totals, pieces):
        up_total, down_total = totals
        normed_rows, hid_rows, act_rows, cot_rows = pieces
        up_term = jnp.dot(normed_rows.T, hid_rows, preferred_element_type=jnp.float32)
        down_term = jnp.dot(act_rows.T, cot_rows, preferred_element_type=jnp.float32)
        up_total = up_total + lax.optimization_barrier(up_term.astype(jnp.bfloat16)).astype(jnp.float32)
        down_total = down_total + lax.optimization_barrier(down_term.astype(jnp.bfloat16)).astype(jnp.float32)
        return ((up_total, down_total), None)
    start_totals = (jnp.zeros((F * RANK, HID), jnp.float32), jnp.zeros((HID, OUT), jnp.float32))
    shard_rows = (normed_b.reshape(N_DP, B_DEV, F * RANK), d_hidden.reshape(N_DP, B_DEV, HID), activated.reshape(N_DP, B_DEV, HID), cotangent.reshape(N_DP, B_DEV, OUT))
    (grad_up, grad_down), unused = lax.scan(add_shard, start_totals, shard_rows)
    d_normed = jnp.dot(d_hidden, up_weight.T, preferred_element_type=jnp.float32)
    grad_fm = inv_rms * (d_normed - normed * lax.optimization_barrier(jnp.mean(d_normed * normed, axis=-1, keepdims=True)))
    grad_cube = grad_fm.reshape(user_count, F, RANK)
    back_proj = jnp.einsum('bfe,bfr->bre', pooled_f32, grad_cube, precision=highest)
    pooled_grad = jnp.einsum('bfr,bre->bfe', grad_cube, mix_f32, precision=highest)
    pooled_grad = pooled_grad + jnp.einsum('fr,bre->bfe', proj_f32, back_proj, precision=highest)
    grad_pooled = pooled_grad.astype(jnp.bfloat16)
    query_terms = lax.map(lambda pieces: query_shard(pieces, score_scale), (ev_blocks, weights, grad_pooled.reshape(N_DP, B_DEV, F, E)))
    grad_query = lax.optimization_barrier(jnp.sum(query_terms, axis=0))
    return (block_out, grad_up, grad_down, grad_pooled, grad_query)
```

```python
import math

import jax
import jax.numpy as jnp
from jax import lax
from jax.experimental import pallas as pl
from jax.experimental.pallas import tpu as pltpu
from jax.sharding import PartitionSpec as P


norm_eps = 1e-05
f32 = jnp.float32
bf16 = jnp.bfloat16


E = 128
L = 8
R = 8
MP = 8
FH = 16
UB = 32
U = 256
NT = (((1,), (1,)), ((), ()))
TN = (((0,), (0,)), ((), ()))
NN = (((1,), (0,)), ((), ()))


def dot(a, b, dims=NN):
    return lax.dot_general(a, b, dims, preferred_element_type=f32)


def iota(shape, axis):
    return lax.broadcasted_iota(jnp.int32, shape, axis)


def own_lanes():
    return iota((FH, E), 0) == iota((FH, E), 1) // L


def group_reduce(x, op):
    lane = iota(x.shape, 1)
    for s in (1, 2, 4):
        up = pltpu.roll(x, E - s, 1)
        down = pltpu.roll(x, s, 1)
        x = op(x, jnp.where((lane & s) == 0, up, down))
    return x


def pool_kernel(ev_ref, len_ref, q_ref, cot_ref, send_ref, w_ref, scr):
    mask = own_lanes()
    raw = dot(q_ref[...], ev_ref[...], NT)
    for u in range(UB):
        block = jnp.where(mask, raw[:, u * E : (u + 1) * E], 0.0)
        scr[u : u + 1, :] = jnp.sum(block, axis=0, keepdims=True)
    scores = scr[...] * (1.0 / math.sqrt(E))
    spread = mask.astype(f32).astype(bf16)
    lens = dot(len_ref[...].astype(f32).astype(bf16), spread)
    live = (iota((UB, E), 1) % L).astype(f32) < lens
    top = group_reduce(jnp.where(live, scores, -1e30), jnp.maximum)
    ex = jnp.exp(jnp.where(live, scores - top, -1e30))
    w = ex / group_reduce(ex, jnp.add)
    w_ref[...] = w
    scr[...] = w
    for u in range(UB):
        row = jnp.broadcast_to(scr[u : u + 1, :], (FH, E))
        mix = jnp.where(mask, row, 0.0).astype(bf16)
        pooled = dot(mix, ev_ref[u * E : (u + 1) * E, :])
        send_ref[0, u * FH : (u + 1) * FH, :] = pooled.astype(bf16)
    send_ref[0, UB * FH :, 0:64] = cot_ref[0 : U // 2, :]
    send_ref[0, UB * FH :, 64:128] = cot_ref[U // 2 :, :]


def pool_call(ev, lens, q, cot):
    rows = UB * FH + U // 2
    return pl.pallas_call(
        pool_kernel,
        grid=(MP,),
        in_specs=[
            pl.BlockSpec((UB * E, E), lambda i: (i, 0)),
            pl.BlockSpec((UB, FH), lambda i: (i, 0)),
            pl.BlockSpec((FH, E), lambda i: (0, 0)),
            pl.BlockSpec((U, 64), lambda i: (0, 0)),
        ],
        out_specs=[
            pl.BlockSpec((1, rows, E), lambda i: (i, 0, 0)),
            pl.BlockSpec((UB, E), lambda i: (i, 0)),
        ],
        out_shape=[
            jax.ShapeDtypeStruct((MP, rows, E), bf16),
            jax.ShapeDtypeStruct((U, E), f32),
        ],
        scratch_shapes=[pltpu.VMEM((UB, E), f32)],
        name="pool",
    )(ev, lens, q, cot)


def flat_mask():
    return iota((E, E), 0) % FH == iota((E, E), 1) // R


def tile_ranks(m):
    pair = jnp.concatenate([m, m], axis=0).astype(bf16)
    return jnp.concatenate([pair] * 8, axis=0)


def user_rows(ref, u):
    return jnp.concatenate(
        [ref[j, pl.ds(pl.multiple_of(u * FH, FH), FH), :] for j in range(MP)], axis=0
    )


def fm_kernel(recv_ref, projt_ref, send_ref, normed_ref, inv_ref, mix_ref, cot_ref, scr):
    mask = flat_mask()
    projt = projt_ref[...]

    def step(u, carry):
        p = user_rows(recv_ref, u)
        mix = dot(projt, p)[0:R].astype(bf16).astype(f32)
        full = jnp.where(mask, dot(p, tile_ranks(mix), NT), 0.0)
        at = pl.multiple_of(u * R, R)
        mix_ref[pl.ds(at, R), :] = mix
        scr[pl.ds(at, R), :] = jnp.sum(full.reshape(MP, FH, E), axis=1)
        return carry

    lax.fori_loop(0, UB, step, 0, unroll=8)
    total = jnp.zeros((UB, 1), f32)
    for j in range(MP):
        x = scr[pl.ds(j, UB, stride=R), :]
        total = total + jnp.sum(x * x, axis=1, keepdims=True)
    inv = lax.rsqrt(total * (1.0 / (E * R)) + norm_eps)
    inv_ref[...] = jnp.broadcast_to(inv, (UB, E))
    for j in range(MP):
        x = scr[pl.ds(j, UB, stride=R), :] * inv
        normed_ref[:, j * E : (j + 1) * E] = x
        for p in range(MP):
            send_ref[p, :, j * E : (j + 1) * E] = x.astype(bf16)
    at = UB * FH
    half = U // 2
    for j in range(MP):
        cot_ref[0:half, j * 64 : (j + 1) * 64] = recv_ref[j, at:, 0:64]
        cot_ref[half:, j * 64 : (j + 1) * 64] = recv_ref[j, at:, 64:128]


def fm_call(recv, projt):
    return pl.pallas_call(
        fm_kernel,
        out_shape=[
            jax.ShapeDtypeStruct((MP, UB, E * R), bf16),
            jax.ShapeDtypeStruct((UB, E * R), f32),
            jax.ShapeDtypeStruct((UB, E), f32),
            jax.ShapeDtypeStruct((UB * R, E), f32),
            jax.ShapeDtypeStruct((U, 512), bf16),
        ],
        scratch_shapes=[pltpu.VMEM((UB * R, E), f32)],
        name="fm_forward",
    )(recv, projt)


HB = 256
STEPS = 4


def layer_step(i, n_ref, cot_ref, up_ref, down_ref, g_ref, out_acc, dn_acc):
    n = n_ref[...]
    cot = cot_ref[...]
    up = up_ref[...]
    down = down_ref[...]
    hidden = dot(n, up)
    d_act = dot(cot, down, NT)
    s = 1.0 / (1.0 + jnp.exp(-hidden))
    act = (hidden * s).astype(bf16)
    d_hidden = (d_act * s * (1.0 + hidden * (1.0 - s))).astype(bf16)
    out_acc[...] += dot(act, down)
    dn_acc[...] += dot(d_hidden, up, NT)
    g_up = dot(n, d_hidden, TN).astype(bf16).reshape(MP, E, HB)
    g_down = dot(act, cot, TN).astype(bf16)
    for k in range(STEPS):

        @pl.when(i == k)
        def _():
            g_ref[:, 0:E, k * HB : (k + 1) * HB] = g_up
            for t in range(2):
                for h in range(2):
                    at = t * 128 + h * 64
                    g_ref[2 * k + t, E : E + 64, h * 512 : (h + 1) * 512] = g_down[at : at + 64, :]


def layer_first(base_ref, rank_ref, n_ref, cot_ref, up_ref, down_ref, g_ref, out_ref, dn_ref):
    i = pl.program_id(0)

    @pl.when(i == 0)
    def _():
        out_ref[...] = jnp.zeros_like(out_ref)
        dn_ref[...] = jnp.zeros_like(dn_ref)

    layer_step(i, n_ref, cot_ref, up_ref, down_ref, g_ref, out_ref, dn_ref)


def layer_second(
    base_ref, rank_ref, n_ref, cot_ref, up_ref, down_ref, out_in, dn_in, g_ref, *refs
):
    sends, (out_acc, dn_acc, packed) = refs[:MP], refs[MP:]
    i = pl.program_id(0)

    @pl.when(i == 0)
    def _():
        out_acc[...] = out_in[...]
        dn_acc[...] = dn_in[...]

    layer_step(i, n_ref, cot_ref, up_ref, down_ref, g_ref, out_acc, dn_acc)

    @pl.when(i == STEPS - 1)
    def _():
        for p in range(MP):
            for g in range(16):
                packed[p, :, g * 64 : (g + 1) * 64] = out_acc[
                    g * 16 : (g + 1) * 16, p * 64 : (p + 1) * 64
                ].astype(bf16)
        for s in range(MP):
            p = rank_ref[0] ^ s
            sends[s][0:UB, :] = dn_acc[pl.ds(pl.multiple_of(p * UB, UB), UB), :].astype(bf16)
            sends[s][UB : UB + 16, :] = packed[p]


def layer_call(base, rank, n, cot, up, down, partial=None):
    whole = lambda shape: pl.BlockSpec(shape, lambda i, b, r: (0,) * len(shape))
    in_specs = [
        whole((U, E * R)),
        whole((U, 512)),
        pl.BlockSpec((E * R, HB), lambda i, b, r: (0, b[0] + i)),
        pl.BlockSpec((HB, 512), lambda i, b, r: (b[0] + i, 0)),
    ]
    args = [n, cot, up, down]
    g_spec, g_shape = whole((MP, 192, 1024)), jax.ShapeDtypeStruct((MP, 192, 1024), bf16)
    acc_shapes = [(U, 512), (U, E * R)]
    if partial is None:
        body, scratch = layer_first, []
        out_specs = [g_spec] + [whole(s) for s in acc_shapes]
        out_shape = [g_shape] + [jax.ShapeDtypeStruct(s, f32) for s in acc_shapes]
    else:
        body, scratch = layer_second, [pltpu.VMEM(s, f32) for s in acc_shapes]
        scratch.append(pltpu.VMEM((MP, 16, 1024), bf16))
        in_specs += [whole(s) for s in acc_shapes]
        args += list(partial)
        out_specs = [g_spec] + [whole((48, 1024))] * MP
        out_shape = [g_shape] + [jax.ShapeDtypeStruct((48, 1024), bf16)] * MP
    return pl.pallas_call(
        body,
        grid_spec=pltpu.PrefetchScalarGridSpec(
            num_scalar_prefetch=2,
            grid=(STEPS,),
            in_specs=in_specs,
            out_specs=out_specs,
            scratch_shapes=scratch,
        ),
        out_shape=out_shape,
        name="layer_first" if partial is None else "layer_second",
    )(base, rank, *args)


def fm_back_kernel(rank_ref, *refs):
    dns = refs[:MP]
    recv_ref, projpad_ref, normed_ref, inv_ref, mix_ref = refs[MP : MP + 5]
    sends = refs[MP + 5 : 2 * MP + 5]
    block_ref, scr, rows = refs[2 * MP + 5 :]
    mask = flat_mask()
    inv = inv_ref[...][:, 0:1]
    dots = jnp.zeros((UB, 1), f32)
    for j in range(MP):
        at = slice(j * E, (j + 1) * E)
        d = dns[0][0:UB, at].astype(f32)
        for s in range(1, MP):
            d = d + dns[s][0:UB, at].astype(f32)
        scr[pl.ds(j, UB, stride=R), :] = d
        dots = dots + jnp.sum(d * normed_ref[:, at], axis=1, keepdims=True)
    mean = dots * (1.0 / (E * R))
    for j in range(MP):
        at = slice(j * E, (j + 1) * E)
        d = scr[pl.ds(j, UB, stride=R), :]
        scr[pl.ds(j, UB, stride=R), :] = inv * (d - normed_ref[:, at] * mean)
    projpad = projpad_ref[...]

    def step(u, carry):
        at = pl.multiple_of(u * R, R)
        p = user_rows(recv_ref, u)
        g = scr[pl.ds(at, R), :]
        spread = jnp.concatenate(
            [jnp.broadcast_to(g[j : j + 1, :], (FH, E)) for j in range(MP)], axis=0
        )
        spread = jnp.where(mask, spread, 0.0).astype(bf16)
        back = jnp.sum(dot(spread, p, TN).reshape(FH, R, E), axis=0)
        high = back.astype(bf16).astype(f32)
        pair = jnp.concatenate([high, back - high], axis=0).astype(bf16)
        back_rows = jnp.concatenate([pair] * 8, axis=0)
        left = jnp.concatenate([spread, projpad], axis=1)
        right = jnp.concatenate([tile_ranks(mix_ref[pl.ds(at, R), :]), back_rows], axis=0)
        grad = dot(left, right).astype(bf16)
        for j in range(MP):
            rows[j, pl.ds(pl.multiple_of(u * FH, FH), FH), :] = grad[j * FH : (j + 1) * FH, :]
        return carry

    lax.fori_loop(0, UB, step, 0, unroll=8)
    for s in range(MP):
        sends[s][...] = rows[rank_ref[0] ^ s]
    out = dns[0][UB : UB + 16, :].astype(f32)
    for s in range(1, MP):
        out = out + dns[s][UB : UB + 16, :].astype(f32)
    out = out.astype(bf16)
    for g in range(16):
        block_ref[g * 16 : (g + 1) * 16, :] = out[:, g * 64 : (g + 1) * 64]


def fm_back_call(rank, dns, recv, projpad, normed, inv, mix):
    args = list(dns) + [recv, projpad, normed, inv, mix]
    whole = lambda shape: pl.BlockSpec(shape, lambda i, r: (0,) * len(shape))
    return pl.pallas_call(
        fm_back_kernel,
        grid_spec=pltpu.PrefetchScalarGridSpec(
            num_scalar_prefetch=1,
            grid=(1,),
            in_specs=[whole(x.shape) for x in args],
            out_specs=[whole((UB * FH, E))] * MP + [whole((U, 64))],
            scratch_shapes=[pltpu.VMEM((UB * R, E), f32), pltpu.VMEM((MP, UB * FH, E), bf16)],
        ),
        out_shape=[jax.ShapeDtypeStruct((UB * FH, E), bf16)] * MP
        + [jax.ShapeDtypeStruct((U, 64), bf16)],
        name="fm_backward",
    )(rank, *args)


def query_kernel(idx_ref, ev_ref, *refs):
    gps, (w_ref, out_ref, pooled_ref, scr, acc) = refs[:MP], refs[MP:]
    i = pl.program_id(0)
    mask = own_lanes()
    for s in range(MP):

        @pl.when(i == s)
        def _():
            pooled_ref[...] = gps[s][...]

    for u in range(UB):
        c = dot(pooled_ref[u * FH : (u + 1) * FH, :], ev_ref[u * E : (u + 1) * E, :], NT)
        scr[u : u + 1, :] = jnp.sum(jnp.where(mask, c, 0.0), axis=0, keepdims=True)
    w = w_ref[...]
    contrib = scr[...]
    d = w * (contrib - group_reduce(w * contrib, jnp.add))
    scr[...] = d
    parts = []
    for u in range(UB):
        row = jnp.broadcast_to(scr[u : u + 1, :], (FH, E))
        parts.append(jnp.where(mask, row, 0.0).astype(bf16))
    term = dot(jnp.concatenate(parts, axis=1), ev_ref[...])

    @pl.when(i == 0)
    def _():
        acc[...] = term

    @pl.when(i > 0)
    def _():
        acc[...] += term

    @pl.when(i == pl.num_programs(0) - 1)
    def _():
        out_ref[...] = acc[...] * (1.0 / math.sqrt(E))


def query_call(idx, ev, gps, w):
    return pl.pallas_call(
        query_kernel,
        grid_spec=pltpu.PrefetchScalarGridSpec(
            num_scalar_prefetch=1,
            grid=(MP,),
            in_specs=[pl.BlockSpec((UB * E, E), lambda i, t: (t[i], 0))]
            + [pl.BlockSpec((UB * FH, E), lambda i, t: (0, 0))] * MP
            + [pl.BlockSpec((UB, E), lambda i, t: (t[i], 0))],
            out_specs=[
                pl.BlockSpec((FH, E), lambda i, t: (0, 0)),
                pl.BlockSpec((UB * FH, E), lambda i, t: (t[i], 0)),
            ],
            scratch_shapes=[pltpu.VMEM((UB, E), f32), pltpu.VMEM((FH, E), f32)],
        ),
        out_shape=[
            jax.ShapeDtypeStruct((FH, E), f32),
            jax.ShapeDtypeStruct((U * FH, E), bf16),
        ],
        name="query_gradient",
    )(idx, ev, *gps, w)


CHUNK = (192, 1024)
HALVES = [jax.ShapeDtypeStruct((1024, 2048), f32), jax.ShapeDtypeStruct((2048, 512), f32)]


def half_kernel(half_ref, stack_ref, *refs):
    part = stack_ref[0]
    up_ref, down_ref = refs[-2:]
    up_ref[...] = part[0:E].astype(f32)
    down_ref[0:64, :] = part[E:, 0:512].astype(f32)
    down_ref[64:128, :] = part[E:, 512:1024].astype(f32)


def half_call(half, stack, outs=()):
    return pl.pallas_call(
        half_kernel,
        grid_spec=pltpu.PrefetchScalarGridSpec(
            num_scalar_prefetch=1,
            grid=(8,),
            in_specs=[pl.BlockSpec((1,) + CHUNK, lambda i, t: (i, 0, 0))]
            + [pl.BlockSpec(memory_space=pl.ANY)] * len(outs),
            out_specs=[
                pl.BlockSpec((E, 1024), lambda i, t: (i, t[0])),
                pl.BlockSpec((E, 512), lambda i, t: (t[0] * 8 + i, 0)),
            ],
        ),
        out_shape=HALVES,
        input_output_aliases={2: 0, 3: 1} if outs else {},
        name="other_half" if outs else "own_half",
    )(half, stack, *outs)


SAME_CORE = [[2 * i + c for i in range(8)] for c in range(2)]


def dp_exchange(x):
    return lax.all_to_all(x, "dp", 0, 0, axis_index_groups=SAME_CORE, tiled=True)


def core_swap(x):
    return lax.ppermute(x, "dp", [(i, i ^ 1) for i in range(16)])


def exchange_slots(xs):
    return [xs[0]] + [
        lax.ppermute(xs[s], "mp", [(i, i ^ s) for i in range(MP)]) for s in range(1, MP)
    ]


def exchange(x):
    return lax.all_to_all(x, "mp", 0, 0, tiled=True)


def device_step(events, lengths, query_vecs, fm_proj, up_weight, down_weight, cotangent):
    c = lax.axis_index("dp") % 2
    m = lax.axis_index("mp")
    ev = events.reshape(U * FH * L, E)
    send, weights = pool_call(ev, lengths, query_vecs, cotangent)
    recv = exchange(send)
    projt = jnp.pad(fm_proj.T, ((0, 8), (0, 0)))
    projpad = jnp.pad(jnp.concatenate([fm_proj, fm_proj], axis=1), ((0, 0), (0, E - 2 * R)))
    rows, normed, inv, mix, cot_full = fm_call(recv, projt)
    n = exchange(rows).reshape(U, E * R)

    other = (1 - c)[None].astype(jnp.int32)
    mine = c[None].astype(jnp.int32)
    rank = m[None].astype(jnp.int32)
    slots = (m ^ jnp.arange(MP)).astype(jnp.int32)
    layer = (rank, n, cot_full, up_weight, down_weight)
    g_other, out_part, dn_part = layer_call(other * STEPS, *layer)
    got = core_swap(g_other)
    g_mine, *dn_sends = layer_call(mine * STEPS, *layer, (out_part, dn_part))
    pair = (g_mine.astype(f32) + got.astype(f32)).astype(bf16)
    parts = dp_exchange(pair)

    dns = exchange_slots(dn_sends)
    *gp_sends, block_out = fm_back_call(rank, dns, recv, projpad, normed, inv, mix)

    chunk = jnp.sum(parts.astype(f32), axis=0).astype(bf16)
    stack = dp_exchange(jnp.broadcast_to(chunk[None], (8,) + CHUNK))

    gps = exchange_slots(gp_sends)
    query_term, grad_pooled = query_call(slots, ev, gps, weights)
    grad_pooled = grad_pooled.reshape(U, FH, E)
    q_all = lax.all_to_all(
        jnp.broadcast_to(query_term.astype(bf16)[None], (16, FH, E)), "dp", 0, 0, tiled=True
    )
    grad_query = jnp.sum(q_all.astype(f32), axis=0)

    stack_other = core_swap(stack)
    halves = half_call(mine, stack)
    grad_up, grad_down = half_call(other, stack_other, halves)
    return (block_out, grad_up, grad_down, grad_pooled, grad_query)


def solution(mesh):
    in_specs = (
        P("dp", "mp", None, None),
        P("dp", "mp"),
        P("mp", None),
        P(),
        P(None, "mp"),
        P("mp", None),
        P("dp", "mp"),
    )
    out_specs = (P("dp", "mp"), P(None, "mp"), P("mp", None), P("dp", "mp", None), P("mp", None))
    return jax.shard_map(
        device_step, mesh=mesh, in_specs=in_specs, out_specs=out_specs, check_vma=False
    )
```

```python
import math

import jax
import jax.numpy as jnp
from jax import lax
from jax.experimental import pallas as pl
from jax.experimental.pallas import tpu as pltpu
from jax.sharding import PartitionSpec as P


norm_eps = 1e-05
f32 = jnp.float32
bf16 = jnp.bfloat16


E = 128
L = 8
R = 8
MP = 8
FH = 16
UB = 32
U = 256
NT = (((1,), (1,)), ((), ()))
TN = (((0,), (0,)), ((), ()))
NN = (((1,), (0,)), ((), ()))


def dot(a, b, dims=NN):
    return lax.dot_general(a, b, dims, preferred_element_type=f32)


def iota(shape, axis):
    return lax.broadcasted_iota(jnp.int32, shape, axis)


def own_lanes():
    return iota((FH, E), 0) == iota((FH, E), 1) // L


def group_reduce(x, op):
    lane = iota(x.shape, 1)
    for s in (1, 2, 4):
        up = pltpu.roll(x, E - s, 1)
        down = pltpu.roll(x, s, 1)
        x = op(x, jnp.where((lane & s) == 0, up, down))
    return x


PARTS = 4
PER = MP // PARTS


def pool_kernel(
    ev_hbm, lent_ref, q_ref, cott_ref, send_hbm, w_hbm, ev, send, w, in_sem, out_sem, w_sem
):
    rows = PER * UB * E
    loads = [
        pltpu.make_async_copy(ev_hbm.at[pl.ds(g * rows, rows)], ev.at[g], in_sem.at[g])
        for g in range(PARTS)
    ]
    for load in loads:
        load.start()
    mask = own_lanes()
    spread = mask.astype(f32).astype(bf16)
    lens = dot(lent_ref[...].astype(f32).astype(bf16), spread, TN)
    live = (iota((U, E), 1) % L).astype(f32) < lens
    q = q_ref[...]
    for g in range(PARTS):
        loads[g].wait()
        raw = dot(q, ev[g], NT)
        for u in range(PER * UB):
            block = jnp.where(mask, raw[:, u * E : (u + 1) * E], 0.0)
            at = g * PER * UB + u
            w[at : at + 1, :] = jnp.sum(block, axis=0, keepdims=True)
    scores = w[...] * (1.0 / math.sqrt(E))
    top = group_reduce(jnp.where(live, scores, -1e30), jnp.maximum)
    ex = jnp.exp(jnp.where(live, scores - top, -1e30))
    w[...] = ex / group_reduce(ex, jnp.add)
    w_copy = pltpu.make_async_copy(w, w_hbm, w_sem)
    w_copy.start()
    stores = []
    for p in range(MP):
        for u in range(UB):
            row = jnp.broadcast_to(w[p * UB + u : p * UB + u + 1, :], (FH, E))
            mix = jnp.where(mask, row, 0.0).astype(bf16)
            at = ((p % PER) * UB + u) * E
            pooled = dot(mix, ev[p // PER, at : at + E, :])
            send[p, u * FH : (u + 1) * FH, :] = pooled.astype(bf16)
        send[p, UB * FH : UB * FH + 64, :] = cott_ref[:, 0:E]
        send[p, UB * FH + 64 :, :] = cott_ref[:, E:]
        stores.append(pltpu.make_async_copy(send.at[p], send_hbm.at[p], out_sem.at[p]))
        stores[-1].start()
    for store in stores:
        store.wait()
    w_copy.wait()


HBM = pl.BlockSpec(memory_space=pltpu.HBM)
VMEM = pl.BlockSpec(memory_space=pltpu.VMEM)


def pool_call(ev, lent, q, cott):
    rows = UB * FH + U // 2
    return pl.pallas_call(
        pool_kernel,
        in_specs=[HBM, VMEM, VMEM, VMEM],
        out_specs=[HBM, HBM],
        out_shape=[
            jax.ShapeDtypeStruct((MP, rows, E), bf16),
            jax.ShapeDtypeStruct((U, E), f32),
        ],
        scratch_shapes=[
            pltpu.VMEM((PARTS, PER * UB * E, E), bf16),
            pltpu.VMEM((MP, rows, E), bf16),
            pltpu.VMEM((U, E), f32),
            pltpu.SemaphoreType.DMA((PARTS,)),
            pltpu.SemaphoreType.DMA((MP,)),
            pltpu.SemaphoreType.DMA,
        ],
        name="pool",
    )(ev, lent, q, cott)


def flat_mask():
    return iota((E, E), 0) % FH == iota((E, E), 1) // R


def tile_ranks(m):
    pair = jnp.concatenate([m, m], axis=0).astype(bf16)
    return jnp.concatenate([pair] * 8, axis=0)


def user_rows(ref, u):
    return jnp.concatenate(
        [ref[j, pl.ds(pl.multiple_of(u * FH, FH), FH), :] for j in range(MP)], axis=0
    )


def fm_kernel(recv_ref, projt_ref, send_ref, normed_ref, inv_ref, mix_ref, cot_ref, scr):
    mask = flat_mask()
    projt = projt_ref[...]

    def step(u, carry):
        p = user_rows(recv_ref, u)
        mix = dot(projt, p)[0:R].astype(bf16).astype(f32)
        full = jnp.where(mask, dot(p, tile_ranks(mix), NT), 0.0)
        at = pl.multiple_of(u * R, R)
        mix_ref[pl.ds(at, R), :] = mix
        scr[pl.ds(at, R), :] = jnp.sum(full.reshape(MP, FH, E), axis=1)
        return carry

    lax.fori_loop(0, UB, step, 0, unroll=16)
    total = jnp.zeros((UB, 1), f32)
    for j in range(MP):
        x = scr[pl.ds(j, UB, stride=R), :]
        total = total + jnp.sum(x * x, axis=1, keepdims=True)
    inv = lax.rsqrt(total * (1.0 / (E * R)) + norm_eps)
    inv_ref[...] = jnp.broadcast_to(inv, (UB, E))
    for j in range(MP):
        x = scr[pl.ds(j, UB, stride=R), :] * inv
        normed_ref[:, j * E : (j + 1) * E] = x
        for p in range(MP):
            send_ref[p, :, j * E : (j + 1) * E] = x.astype(bf16)
    at = UB * FH
    for j in range(MP):
        cot_ref[j * 64 : (j + 1) * 64, 0:E] = recv_ref[j, at : at + 64, :]
        cot_ref[j * 64 : (j + 1) * 64, E:] = recv_ref[j, at + 64 :, :]


def fm_call(recv, projt):
    return pl.pallas_call(
        fm_kernel,
        out_shape=[
            jax.ShapeDtypeStruct((MP, UB, E * R), bf16),
            jax.ShapeDtypeStruct((UB, E * R), f32),
            jax.ShapeDtypeStruct((UB, E), f32),
            jax.ShapeDtypeStruct((UB * R, E), f32),
            jax.ShapeDtypeStruct((512, U), bf16),
        ],
        scratch_shapes=[pltpu.VMEM((UB * R, E), f32)],
        name="fm_forward",
    )(recv, projt)


HB = 256
STEPS = 4
HALF = HB * STEPS


def weight_loads(half, up_hbm, down_hbm, up, down, sem):
    loads = []
    for k in range(STEPS):
        at = pl.multiple_of(half * HALF + k * HB, HB)
        here = pl.ds(k * HB, HB)
        loads.append(
            (
                pltpu.make_async_copy(up_hbm.at[:, pl.ds(at, HB)], up.at[:, here], sem.at[0, k]),
                pltpu.make_async_copy(down_hbm.at[pl.ds(at, HB)], down.at[here], sem.at[1, k]),
            )
        )
    return loads


def start_all(copies):
    for copy in copies:
        copy.start()


def wait_all(copies):
    for copy in copies:
        copy.wait()


def layer_half(loads, n, nt, cot, up, down, act, dh, g, g_hbm, sem):
    stores = []
    for k in range(STEPS):
        wait_all(loads[k])
        cols = slice(k * HB, (k + 1) * HB)
        hidden = dot(n, up[:, cols])
        d_act = dot(cot, down[cols, :], NT)
        s = 1.0 / (1.0 + jnp.exp(-hidden))
        act_k = (hidden * s).astype(bf16)
        dh_k = (d_act * s * (1.0 + hidden * (1.0 - s))).astype(bf16)
        act[:, cols] = act_k
        dh[:, cols] = dh_k
        g[:, 0:E, cols] = dot(nt, dh_k).astype(bf16).reshape(MP, E, HB)
        g_down = dot(act_k, cot, TN).astype(bf16)
        for t in range(2):
            for h in range(2):
                at = t * 128 + h * 64
                g[2 * k + t, E:, h * 512 : (h + 1) * 512] = g_down[at : at + 64, :]
        here = pl.ds(k * HB, HB)
        pair = pl.ds(2 * k, 2)
        low = pl.ds(E, 64)
        stores += [
            pltpu.make_async_copy(
                g.at[:, pl.ds(0, E), here], g_hbm.at[:, pl.ds(0, E), here], sem.at[0, k]
            ),
            pltpu.make_async_copy(g.at[pair, low], g_hbm.at[pair, low], sem.at[1, k]),
        ]
        start_all(stores[-2:])
    return stores


def layer_first(
    half_ref, n_hbm, cott_hbm, up_hbm, down_hbm, g_hbm, act_hbm, dh_hbm,
    n, nt, cott, up, down, act, dh, g, in_sem, w_sem, g_sem, out_sem,
):
    first = [
        pltpu.make_async_copy(n_hbm, n, in_sem.at[0]),
        pltpu.make_async_copy(cott_hbm, cott, in_sem.at[1]),
    ]
    loads = weight_loads(half_ref[0], up_hbm, down_hbm, up, down, w_sem)
    start_all(first)
    for pair in loads:
        start_all(pair)
    wait_all(first)
    rows = n[...]
    nt[...] = rows.T
    cot = cott[...].T
    stores = layer_half(loads, rows, nt[...], cot, up, down, act, dh, g, g_hbm, g_sem)
    last = [
        pltpu.make_async_copy(act, act_hbm, out_sem.at[0]),
        pltpu.make_async_copy(dh, dh_hbm, out_sem.at[1]),
    ]
    start_all(last)
    wait_all(stores)
    wait_all(last)


def layer_second(
    half_ref, n_hbm, cott_hbm, up_hbm, down_hbm, act_hbm, dh_hbm, g_hbm, *refs
):
    sends = refs[:MP]
    n, nt, cott, up, down, act, dh, g, in_sem, w_sem, g_sem = refs[MP : MP + 11]
    up_o, down_o, act_o, dh_o, dn, packed, wo_sem = refs[MP + 11 :]
    first = [
        pltpu.make_async_copy(n_hbm, n, in_sem.at[0]),
        pltpu.make_async_copy(cott_hbm, cott, in_sem.at[1]),
    ]
    half = half_ref[0]
    loads = weight_loads(half, up_hbm, down_hbm, up, down, w_sem)
    others = weight_loads(1 - half, up_hbm, down_hbm, up_o, down_o, wo_sem)
    late = [
        pltpu.make_async_copy(act_hbm, act_o, in_sem.at[2]),
        pltpu.make_async_copy(dh_hbm, dh_o, in_sem.at[3]),
    ]
    for pair in others:
        late += pair
    start_all(first)
    for pair in loads:
        start_all(pair)
    start_all(late)
    wait_all(first)
    rows = n[...]
    nt[...] = rows.T
    cot = cott[...].T
    stores = layer_half(loads, rows, nt[...], cot, up, down, act, dh, g, g_hbm, g_sem)
    wait_all(late)
    out = dot(act[...], down[...]) + dot(act_o[...], down_o[...])
    out = out.T
    for p in range(MP):
        for a in range(4):
            at = p * 64 + a * 16
            packed[p, :, a * U : (a + 1) * U] = out[at : at + 16, :].astype(bf16)
    dn[...] = dot(dh[...], up[...], NT) + dot(dh_o[...], up_o[...], NT)
    for s in range(MP):
        p = half_ref[1] ^ s
        sends[s][0:UB, :] = dn[pl.ds(pl.multiple_of(p * UB, UB), UB), :].astype(bf16)
        sends[s][UB:, :] = packed[p]
    wait_all(stores)


def layer_call(half, n, cott, up, down, others=()):
    wide, tall = pltpu.VMEM((E * R, HALF), bf16), pltpu.VMEM((HALF, 512), bf16)
    slab = pltpu.VMEM((U, HALF), bf16)
    sems = lambda *shape: pltpu.SemaphoreType.DMA(shape)
    scratch = [
        pltpu.VMEM((U, E * R), bf16),
        pltpu.VMEM((E * R, U), bf16),
        pltpu.VMEM((512, U), bf16),
        wide, tall, slab, slab,
        pltpu.VMEM((MP, 192, 1024), bf16),
    ]
    g_shape = jax.ShapeDtypeStruct((MP, 192, 1024), bf16)
    if others:
        body = layer_second
        scratch += [sems(4), sems(2, STEPS), sems(2, STEPS)]
        scratch += [wide, tall, slab, slab, pltpu.VMEM((U, E * R), f32)]
        scratch += [pltpu.VMEM((MP, 16, 1024), bf16), sems(2, STEPS)]
        out_specs = [HBM] + [VMEM] * MP
        out_shape = [g_shape] + [jax.ShapeDtypeStruct((48, 1024), bf16)] * MP
    else:
        body = layer_first
        scratch += [sems(2), sems(2, STEPS), sems(2, STEPS), sems(2)]
        out_specs = [HBM] * 3
        out_shape = [g_shape] + [jax.ShapeDtypeStruct((U, HALF), bf16)] * 2
    return pl.pallas_call(
        body,
        in_specs=[pl.BlockSpec(memory_space=pltpu.SMEM)] + [HBM] * (4 + len(others)),
        out_specs=out_specs,
        out_shape=out_shape,
        scratch_shapes=scratch,
        name="layer_second" if others else "layer_first",
    )(half, n, cott, up, down, *others)


def fm_back_kernel(rank_ref, *refs):
    dns = refs[:MP]
    recv_ref, projpad_ref, normed_ref, inv_ref, mix_ref = refs[MP : MP + 5]
    sends = refs[MP + 5 : 2 * MP + 5]
    block_ref, scr, rows = refs[2 * MP + 5 :]
    mask = flat_mask()
    inv = inv_ref[...][:, 0:1]
    dots = jnp.zeros((UB, 1), f32)
    for j in range(MP):
        at = slice(j * E, (j + 1) * E)
        d = dns[0][0:UB, at].astype(f32)
        for s in range(1, MP):
            d = d + dns[s][0:UB, at].astype(f32)
        scr[pl.ds(j, UB, stride=R), :] = d
        dots = dots + jnp.sum(d * normed_ref[:, at], axis=1, keepdims=True)
    mean = dots * (1.0 / (E * R))
    for j in range(MP):
        at = slice(j * E, (j + 1) * E)
        d = scr[pl.ds(j, UB, stride=R), :]
        scr[pl.ds(j, UB, stride=R), :] = inv * (d - normed_ref[:, at] * mean)
    projpad = projpad_ref[...]

    def step(u, carry):
        at = pl.multiple_of(u * R, R)
        p = user_rows(recv_ref, u)
        g = scr[pl.ds(at, R), :]
        spread = jnp.concatenate(
            [jnp.broadcast_to(g[j : j + 1, :], (FH, E)) for j in range(MP)], axis=0
        )
        spread = jnp.where(mask, spread, 0.0).astype(bf16)
        back = jnp.sum(dot(spread, p, TN).reshape(FH, R, E), axis=0)
        high = back.astype(bf16).astype(f32)
        pair = jnp.concatenate([high, back - high], axis=0).astype(bf16)
        back_rows = jnp.concatenate([pair] * 8, axis=0)
        left = jnp.concatenate([spread, projpad], axis=1)
        right = jnp.concatenate([tile_ranks(mix_ref[pl.ds(at, R), :]), back_rows], axis=0)
        grad = dot(left, right).astype(bf16)
        for j in range(MP):
            rows[j, pl.ds(pl.multiple_of(u * FH, FH), FH), :] = grad[j * FH : (j + 1) * FH, :]
        return carry

    lax.fori_loop(0, UB, step, 0, unroll=16)
    for s in range(MP):
        sends[s][...] = rows[rank_ref[0] ^ s]
    out = dns[0][UB : UB + 16, :].astype(f32)
    for s in range(1, MP):
        out = out + dns[s][UB : UB + 16, :].astype(f32)
    out = out.astype(bf16)
    for a in range(4):
        block_ref[a * 16 : (a + 1) * 16, :] = out[:, a * U : (a + 1) * U]


def fm_back_call(rank, dns, recv, projpad, normed, inv, mix):
    args = list(dns) + [recv, projpad, normed, inv, mix]
    whole = lambda shape: pl.BlockSpec(shape, lambda i, r: (0,) * len(shape))
    return pl.pallas_call(
        fm_back_kernel,
        grid_spec=pltpu.PrefetchScalarGridSpec(
            num_scalar_prefetch=1,
            grid=(1,),
            in_specs=[whole(x.shape) for x in args],
            out_specs=[whole((UB * FH, E))] * MP + [whole((64, U))],
            scratch_shapes=[pltpu.VMEM((UB * R, E), f32), pltpu.VMEM((MP, UB * FH, E), bf16)],
        ),
        out_shape=[jax.ShapeDtypeStruct((UB * FH, E), bf16)] * MP
        + [jax.ShapeDtypeStruct((64, U), bf16)],
        name="fm_backward",
    )(rank, *args)


def query_kernel(idx_ref, ev_ref, *refs):
    gps, (w_ref, out_ref, pooled_ref, scr, acc) = refs[:MP], refs[MP:]
    i = pl.program_id(0)
    mask = own_lanes()
    for s in range(MP):

        @pl.when(i == s)
        def _():
            pooled_ref[...] = gps[s][...]

    for u in range(UB):
        c = dot(pooled_ref[u * FH : (u + 1) * FH, :], ev_ref[u * E : (u + 1) * E, :], NT)
        scr[u : u + 1, :] = jnp.sum(jnp.where(mask, c, 0.0), axis=0, keepdims=True)
    w = w_ref[...]
    contrib = scr[...]
    d = w * (contrib - group_reduce(w * contrib, jnp.add))
    scr[...] = d
    parts = []
    for u in range(UB):
        row = jnp.broadcast_to(scr[u : u + 1, :], (FH, E))
        parts.append(jnp.where(mask, row, 0.0).astype(bf16))
    term = dot(jnp.concatenate(parts, axis=1), ev_ref[...])

    @pl.when(i == 0)
    def _():
        acc[...] = term

    @pl.when(i > 0)
    def _():
        acc[...] += term

    @pl.when(i == pl.num_programs(0) - 1)
    def _():
        out_ref[...] = acc[...] * (1.0 / math.sqrt(E))


def query_call(idx, ev, gps, w):
    return pl.pallas_call(
        query_kernel,
        grid_spec=pltpu.PrefetchScalarGridSpec(
            num_scalar_prefetch=1,
            grid=(MP,),
            in_specs=[pl.BlockSpec((UB * E, E), lambda i, t: (t[i], 0))]
            + [pl.BlockSpec((UB * FH, E), lambda i, t: (0, 0))] * MP
            + [pl.BlockSpec((UB, E), lambda i, t: (t[i], 0))],
            out_specs=[
                pl.BlockSpec((FH, E), lambda i, t: (0, 0)),
                pl.BlockSpec((UB * FH, E), lambda i, t: (t[i], 0)),
            ],
            scratch_shapes=[pltpu.VMEM((UB, E), f32), pltpu.VMEM((FH, E), f32)],
        ),
        out_shape=[
            jax.ShapeDtypeStruct((FH, E), f32),
            jax.ShapeDtypeStruct((U * FH, E), bf16),
        ],
        name="query_gradient",
    )(idx, ev, *gps, w)


CHUNK = (192, 1024)
HALVES = [jax.ShapeDtypeStruct((1024, 2048), f32), jax.ShapeDtypeStruct((2048, 512), f32)]


def half_kernel(half_ref, stack_hbm, *refs):
    up_hbm, down_hbm, stack, up, down, in_sem, up_sem, down_sem = refs[-8:]
    loads = [
        pltpu.make_async_copy(stack_hbm.at[i], stack.at[i], in_sem.at[i]) for i in range(8)
    ]
    start_all(loads)
    cols = pl.ds(pl.multiple_of(half_ref[0] * HALF, HALF), HALF)
    stores = []
    for i in range(8):
        loads[i].wait()
        at = i * E
        up[at : at + E, :] = stack[i, 0:E, :].astype(f32)
        down[at : at + 64, :] = stack[i, E:, 0:512].astype(f32)
        down[at + 64 : at + E, :] = stack[i, E:, 512:].astype(f32)
        rows = pl.ds(at, E)
        out_rows = pl.ds(pl.multiple_of(half_ref[0] * HALF + at, E), E)
        stores += [
            pltpu.make_async_copy(up.at[rows], up_hbm.at[rows, cols], up_sem.at[i]),
            pltpu.make_async_copy(down.at[rows], down_hbm.at[out_rows], down_sem.at[i]),
        ]
        start_all(stores[-2:])
    wait_all(stores)


def half_call(half, stack, outs=()):
    return pl.pallas_call(
        half_kernel,
        in_specs=[pl.BlockSpec(memory_space=pltpu.SMEM)] + [HBM] * (1 + len(outs)),
        out_specs=[HBM, HBM],
        out_shape=HALVES,
        scratch_shapes=[
            pltpu.VMEM((8,) + CHUNK, bf16),
            pltpu.VMEM((1024, 1024), f32),
            pltpu.VMEM((1024, 512), f32),
        ]
        + [pltpu.SemaphoreType.DMA((8,))] * 3,
        input_output_aliases={2: 0, 3: 1} if outs else {},
        name="other_half" if outs else "own_half",
    )(half, stack, *outs)


SAME_CORE = [[2 * i + c for i in range(8)] for c in range(2)]


def dp_exchange(x):
    return lax.all_to_all(x, "dp", 0, 0, axis_index_groups=SAME_CORE, tiled=True)


def core_swap(x):
    return lax.ppermute(x, "dp", [(i, i ^ 1) for i in range(16)])


def exchange_slots(xs):
    got = [xs[0]]
    for s in range(1, MP):
        got.append(lax.ppermute(xs[s], "mp", [(i, i ^ s) for i in range(MP)]))
    return got


def dp_permute(x, s):
    pairs = [
        (h * 8 + z * 2 + c, (h ^ (s // 4)) * 8 + ((z + s) % 4) * 2 + c)
        for h in range(2)
        for z in range(4)
        for c in range(2)
    ]
    return lax.ppermute(x, "dp", pairs)


def exchange(x):
    return lax.all_to_all(x, "mp", 0, 0, tiled=True)


def device_step(events, lengths, query_vecs, fm_proj, up_weight, down_weight, cotangent):
    c = lax.axis_index("dp") % 2
    m = lax.axis_index("mp")
    ev = events.reshape(U * FH * L, E)
    send, weights = pool_call(ev, lengths.T, query_vecs, cotangent.T)
    recv = exchange(send)
    projt = jnp.pad(fm_proj.T, ((0, 8), (0, 0)))
    projpad = jnp.pad(jnp.concatenate([fm_proj, fm_proj], axis=1), ((0, 0), (0, E - 2 * R)))
    rows, normed, inv, mix, cot_full = fm_call(recv, projt)
    n = exchange(rows).reshape(U, E * R)

    other = (1 - c)[None].astype(jnp.int32)
    mine = c[None].astype(jnp.int32)
    rank = m[None].astype(jnp.int32)
    slots = (m ^ jnp.arange(MP)).astype(jnp.int32)
    layer = (n, cot_full, up_weight, down_weight)
    g_other, *others = layer_call(other, *layer)
    got = core_swap(g_other)
    g_mine, *dn_sends = layer_call(jnp.concatenate([mine, rank]), *layer, tuple(others))
    pair = (g_mine.astype(f32) + got.astype(f32)).astype(bf16)
    parts = dp_exchange(pair)

    dns = exchange_slots(dn_sends)
    *gp_sends, block_out = fm_back_call(rank, dns, recv, projpad, normed, inv, mix)

    chunk = jnp.sum(parts.astype(f32), axis=0).astype(bf16)
    stack = dp_exchange(jnp.broadcast_to(chunk[None], (8,) + CHUNK))

    gps = exchange_slots(gp_sends)
    query_term, grad_pooled = query_call(slots, ev, gps, weights)
    grad_pooled = grad_pooled.reshape(U, FH, E)
    query_other = core_swap(query_term)
    query_pair = (query_term + query_other).astype(bf16)
    query_parts = [query_pair] + [dp_permute(query_pair, s) for s in range(1, 8)]
    grad_query = sum(x.astype(f32) for x in query_parts)

    stack_other = core_swap(stack)
    halves = half_call(mine, stack)
    grad_up, grad_down = half_call(other, stack_other, halves)
    return (block_out.T, grad_up, grad_down, grad_pooled, grad_query)


def solution(mesh):
    in_specs = (
        P("dp", "mp", None, None),
        P("dp", "mp"),
        P("mp", None),
        P(),
        P(None, "mp"),
        P("mp", None),
        P("dp", "mp"),
    )
    out_specs = (P("dp", "mp"), P(None, "mp"), P("mp", None), P("dp", "mp", None), P("mp", None))
    return jax.shard_map(
        device_step, mesh=mesh, in_specs=in_specs, out_specs=out_specs, check_vma=False
    )
```

```python
import math

import jax
import jax.numpy as jnp
from jax import lax
from jax.experimental import pallas as pl
from jax.experimental.pallas import tpu as pltpu
from jax.sharding import PartitionSpec as P


norm_eps = 1e-05
f32 = jnp.float32
bf16 = jnp.bfloat16


E = 128
L = 8
R = 8
MP = 8
FH = 16
UB = 32
U = 256
NT = (((1,), (1,)), ((), ()))
TN = (((0,), (0,)), ((), ()))
NN = (((1,), (0,)), ((), ()))


def dot(a, b, dims=NN):
    return lax.dot_general(a, b, dims, preferred_element_type=f32)


def iota(shape, axis):
    return lax.broadcasted_iota(jnp.int32, shape, axis)


def own_lanes():
    return iota((FH, E), 0) == iota((FH, E), 1) // L


def group_reduce(x, op):
    lane = iota(x.shape, 1)
    for s in (1, 2, 4):
        up = pltpu.roll(x, E - s, 1)
        down = pltpu.roll(x, s, 1)
        x = op(x, jnp.where((lane & s) == 0, up, down))
    return x


PARTS = 2
PER = MP // PARTS


def pool_kernel(
    ev_hbm, lent_ref, q_ref, cott_ref, send_hbm, w_hbm, ev, send, w, in_sem, out_sem, w_sem
):
    rows = PER * UB * E
    loads = [
        pltpu.make_async_copy(ev_hbm.at[pl.ds(g * rows, rows)], ev.at[g], in_sem.at[g])
        for g in range(PARTS)
    ]
    for load in loads:
        load.start()
    mask = own_lanes()
    spread = mask.astype(f32).astype(bf16)
    lens = dot(lent_ref[...].astype(f32).astype(bf16), spread, TN)
    live = (iota((U, E), 1) % L).astype(f32) < lens
    q = q_ref[...]
    copies = []
    for g in range(PARTS):
        loads[g].wait()
        raw = dot(q, ev[g], NT)
        first = g * PER * UB
        here = slice(first, first + PER * UB)
        for u in range(PER * UB):
            block = jnp.where(mask, raw[:, u * E : (u + 1) * E], 0.0)
            w[first + u : first + u + 1, :] = jnp.sum(block, axis=0, keepdims=True)
        scores = w[here, :] * (1.0 / math.sqrt(E))
        top = group_reduce(jnp.where(live[here], scores, -1e30), jnp.maximum)
        ex = jnp.exp(jnp.where(live[here], scores - top, -1e30))
        w[here, :] = ex / group_reduce(ex, jnp.add)
        for i in range(PER):
            p = g * PER + i
            for u in range(UB):
                row = jnp.broadcast_to(w[p * UB + u : p * UB + u + 1, :], (FH, E))
                weight = jnp.where(mask, row, 0.0).astype(bf16)
                at = (i * UB + u) * E
                pooled = dot(weight, ev[g, at : at + E, :])
                send[p, u * FH : (u + 1) * FH, :] = pooled.astype(bf16)
            send[p, UB * FH : UB * FH + 64, :] = cott_ref[:, 0:E]
            send[p, UB * FH + 64 :, :] = cott_ref[:, E:]
            copies.append(pltpu.make_async_copy(send.at[p], send_hbm.at[p], out_sem.at[p]))
            copies[-1].start()
    copies.append(pltpu.make_async_copy(w, w_hbm, w_sem))
    copies[-1].start()
    wait_all(copies)


HBM = pl.BlockSpec(memory_space=pltpu.HBM)
VMEM = pl.BlockSpec(memory_space=pltpu.VMEM)


def pool_call(ev, lent, q, cott):
    rows = UB * FH + U // 2
    return pl.pallas_call(
        pool_kernel,
        in_specs=[HBM, VMEM, VMEM, VMEM],
        out_specs=[HBM, HBM],
        out_shape=[
            jax.ShapeDtypeStruct((MP, rows, E), bf16),
            jax.ShapeDtypeStruct((U, E), f32),
        ],
        scratch_shapes=[
            pltpu.VMEM((PARTS, PER * UB * E, E), bf16),
            pltpu.VMEM((MP, rows, E), bf16),
            pltpu.VMEM((U, E), f32),
            pltpu.SemaphoreType.DMA((PARTS,)),
            pltpu.SemaphoreType.DMA((MP,)),
            pltpu.SemaphoreType.DMA,
        ],
        name="pool",
    )(ev, lent, q, cott)


def flat_mask():
    return iota((E, E), 0) % FH == iota((E, E), 1) // R


def tile_ranks(m):
    pair = jnp.concatenate([m, m], axis=0).astype(bf16)
    return jnp.concatenate([pair] * 8, axis=0)


def user_rows(ref, u):
    return jnp.concatenate(
        [ref[j, pl.ds(pl.multiple_of(u * FH, FH), FH), :] for j in range(MP)], axis=0
    )


def fm_kernel(recv_ref, projt_ref, *refs):
    outs, (rows, normed, inv_v, mix_v, cot, scr, row_sem, sem) = refs[:5], refs[5:]
    mask = flat_mask()
    projt = projt_ref[...]
    at = UB * FH
    for j in range(MP):
        cot[j * 64 : (j + 1) * 64, 0:E] = recv_ref[j, at : at + 64, :]
        cot[j * 64 : (j + 1) * 64, E:] = recv_ref[j, at + 64 :, :]
    copies = [
        pltpu.make_async_copy(v, o, sem.at[i])
        for i, (v, o) in enumerate(zip((normed, inv_v, mix_v, cot), outs[1:]))
    ]
    copies[3].start()

    def step(u, carry):
        p = user_rows(recv_ref, u)
        mix = dot(projt, p)[0:R].astype(bf16).astype(f32)
        full = jnp.where(mask, dot(p, tile_ranks(mix), NT), 0.0)
        at = pl.multiple_of(u * R, R)
        mix_v[pl.ds(at, R), :] = mix
        scr[pl.ds(at, R), :] = jnp.sum(full.reshape(MP, FH, E), axis=1)
        return carry

    lax.fori_loop(0, UB, step, 0, unroll=32)
    copies[2].start()
    total = jnp.zeros((UB, 1), f32)
    for j in range(MP):
        x = scr[pl.ds(j, UB, stride=R), :]
        total = total + jnp.sum(x * x, axis=1, keepdims=True)
    inv = lax.rsqrt(total * (1.0 / (E * R)) + norm_eps)
    inv_v[...] = jnp.broadcast_to(inv, (UB, E))
    for j in range(MP):
        x = scr[pl.ds(j, UB, stride=R), :] * inv
        normed[:, j * E : (j + 1) * E] = x
        rows[:, j * E : (j + 1) * E] = x.astype(bf16)
    copies += [pltpu.make_async_copy(rows, outs[0].at[p], row_sem.at[p]) for p in range(MP)]
    start_all(copies[4:])
    start_all(copies[:2])
    wait_all(copies)


def fm_call(recv, projt):
    return pl.pallas_call(
        fm_kernel,
        in_specs=[VMEM, VMEM],
        out_specs=[HBM] * 5,
        out_shape=[
            jax.ShapeDtypeStruct((MP, UB, E * R), bf16),
            jax.ShapeDtypeStruct((UB, E * R), f32),
            jax.ShapeDtypeStruct((UB, E), f32),
            jax.ShapeDtypeStruct((UB * R, E), f32),
            jax.ShapeDtypeStruct((512, U), bf16),
        ],
        scratch_shapes=[
            pltpu.VMEM((UB, E * R), bf16),
            pltpu.VMEM((UB, E * R), f32),
            pltpu.VMEM((UB, E), f32),
            pltpu.VMEM((UB * R, E), f32),
            pltpu.VMEM((512, U), bf16),
            pltpu.VMEM((UB * R, E), f32),
            pltpu.SemaphoreType.DMA((MP,)),
            pltpu.SemaphoreType.DMA((4,)),
        ],
        name="fm_forward",
    )(recv, projt)


HB = 256
STEPS = 4
HALF = HB * STEPS


def weight_loads(half, up_hbm, down_hbm, up, down, sem, k):
    at = pl.multiple_of(half * HALF + k * HB, HB)
    here = pl.ds(pl.multiple_of(k * HB, HB), HB)
    return [
        pltpu.make_async_copy(up_hbm.at[:, pl.ds(at, HB)], up.at[:, here], sem.at[0, k]),
        pltpu.make_async_copy(down_hbm.at[pl.ds(at, HB)], down.at[here], sem.at[1, k]),
    ]


def start_all(copies):
    for copy in copies:
        copy.start()


def wait_all(copies):
    for copy in copies:
        copy.wait()


def gradient_stores(g, g_hbm, sem, k):
    here = pl.ds(pl.multiple_of(k * HB, HB), HB)
    pair = pl.ds(2 * k, 2)
    low = pl.ds(E, 64)
    return [
        pltpu.make_async_copy(
            g.at[:, pl.ds(0, E), here], g_hbm.at[:, pl.ds(0, E), here], sem.at[0, k]
        ),
        pltpu.make_async_copy(g.at[pair, low], g_hbm.at[pair, low], sem.at[1, k]),
    ]


def layer_half(loads, stores, n, nt, cot, up, down, act, dh, g):
    def block(k, carry):
        wait_all(loads(k))
        cols = pl.ds(pl.multiple_of(k * HB, HB), HB)
        hidden = dot(n[...], up[:, cols])
        d_act = dot(cot[...], down[cols, :], NT)
        s = 1.0 / (1.0 + jnp.exp(-hidden))
        act_k = (hidden * s).astype(bf16)
        dh_k = (d_act * s * (1.0 + hidden * (1.0 - s))).astype(bf16)
        act[:, cols] = act_k
        dh[:, cols] = dh_k
        g[:, 0:E, cols] = dot(nt[...], dh_k).astype(bf16).reshape(MP, E, HB)
        g_down = dot(act_k, cot[...], TN).astype(bf16)
        for t in range(2):
            for h in range(2):
                at = t * 128 + h * 64
                g[2 * k + t, E:, h * 512 : (h + 1) * 512] = g_down[at : at + 64, :]
        start_all(stores(k))
        return carry

    lax.fori_loop(0, STEPS, block, 0)


def layer_first(
    half_ref, rank_ref, n_hbm, cott_hbm, up_hbm, down_hbm, g_hbm, act_hbm, dh_hbm,
    n, nt, cott, cot, up, down, act, dh, g, in_sem, w_sem, g_sem, out_sem,
):
    first = [
        pltpu.make_async_copy(n_hbm, n, in_sem.at[0]),
        pltpu.make_async_copy(cott_hbm, cott, in_sem.at[1]),
    ]
    loads = lambda k: weight_loads(half_ref[0], up_hbm, down_hbm, up, down, w_sem, k)
    stores = lambda k: gradient_stores(g, g_hbm, g_sem, k)
    start_all(first)
    for k in range(STEPS):
        start_all(loads(k))
    wait_all(first)
    nt[...] = n[...].T
    cot[...] = cott[...].T
    layer_half(loads, stores, n, nt, cot, up, down, act, dh, g)
    last = [
        pltpu.make_async_copy(act, act_hbm, out_sem.at[0]),
        pltpu.make_async_copy(dh, dh_hbm, out_sem.at[1]),
    ]
    start_all(last)
    for k in range(STEPS):
        wait_all(stores(k))
    wait_all(last)


def layer_second(
    half_ref, rank_ref, n_hbm, cott_hbm, up_hbm, down_hbm, act_hbm, dh_hbm, g_hbm, cross, keep, *refs
):
    n, nt, cott, cot, up, down, act, dh, g, in_sem, w_sem, g_sem = refs[:12]
    up_o, down_o, act_o, dh_o, dn, packed, wo_sem = refs[12:]
    first = [
        pltpu.make_async_copy(n_hbm, n, in_sem.at[0]),
        pltpu.make_async_copy(cott_hbm, cott, in_sem.at[1]),
    ]
    half = half_ref[0]
    loads = lambda k: weight_loads(half, up_hbm, down_hbm, up, down, w_sem, k)
    stores = lambda k: gradient_stores(g, g_hbm, g_sem, k)
    late = [
        pltpu.make_async_copy(act_hbm, act_o, in_sem.at[2]),
        pltpu.make_async_copy(dh_hbm, dh_o, in_sem.at[3]),
    ]
    for k in range(STEPS):
        late += weight_loads(1 - half, up_hbm, down_hbm, up_o, down_o, wo_sem, k)
    start_all(first)
    for k in range(STEPS):
        start_all(loads(k))
    start_all(late)
    wait_all(first)
    nt[...] = n[...].T
    cot[...] = cott[...].T
    layer_half(loads, stores, n, nt, cot, up, down, act, dh, g)
    wait_all(late)
    out = dot(act[...], down[...]) + dot(act_o[...], down_o[...])
    out = out.T
    for p in range(MP):
        for a in range(4):
            at = p * 64 + a * 16
            packed[p, :, a * U : (a + 1) * U] = out[at : at + 16, :].astype(bf16)
    dn[...] = dot(dh[...], up[...], NT) + dot(dh_o[...], up_o[...], NT)
    for k in range(4):
        for flip, to in ((1, cross), (0, keep)):
            p = rank_ref[0] ^ flip ^ (2 * k)
            to[k, 0:UB, :] = dn[pl.ds(pl.multiple_of(p * UB, UB), UB), :].astype(bf16)
            to[k, UB:, :] = packed[p]
    for k in range(STEPS):
        wait_all(stores(k))


def layer_call(half, rank, n, cott, up, down, others=()):
    wide, tall = pltpu.VMEM((E * R, HALF), bf16), pltpu.VMEM((HALF, 512), bf16)
    slab = pltpu.VMEM((U, HALF), bf16)
    sems = lambda *shape: pltpu.SemaphoreType.DMA(shape)
    scratch = [
        pltpu.VMEM((U, E * R), bf16),
        pltpu.VMEM((E * R, U), bf16),
        pltpu.VMEM((512, U), bf16),
        pltpu.VMEM((U, 512), bf16),
        wide, tall, slab, slab,
        pltpu.VMEM((MP, 192, 1024), bf16),
    ]
    g_shape = jax.ShapeDtypeStruct((MP, 192, 1024), bf16)
    if others:
        body = layer_second
        scratch += [sems(4), sems(2, STEPS), sems(2, STEPS)]
        scratch += [wide, tall, slab, slab, pltpu.VMEM((U, E * R), f32)]
        scratch += [pltpu.VMEM((MP, 16, 1024), bf16), sems(2, STEPS)]
        out_specs = [HBM] + [VMEM] * 2
        out_shape = [g_shape] + [jax.ShapeDtypeStruct((4, 48, 1024), bf16)] * 2
    else:
        body = layer_first
        scratch += [sems(2), sems(2, STEPS), sems(2, STEPS), sems(2)]
        out_specs = [HBM] * 3
        out_shape = [g_shape] + [jax.ShapeDtypeStruct((U, HALF), bf16)] * 2
    return pl.pallas_call(
        body,
        in_specs=[pl.BlockSpec(memory_space=pltpu.SMEM)] * 2 + [HBM] * (4 + len(others)),
        out_specs=out_specs,
        out_shape=out_shape,
        scratch_shapes=scratch,
        name="layer_second" if others else "layer_first",
    )(half, rank, n, cott, up, down, *others)


def pair_kernel(own, got, out_hbm, total, sem):
    stores = [pltpu.make_async_copy(total.at[t], out_hbm.at[t], sem.at[t]) for t in range(8)]
    for t in range(8):
        total[t] = (own[t].astype(f32) + got[t].astype(f32)).astype(bf16)
        stores[t].start()
    wait_all(stores)


def pair_call(own, got):
    shape = (8, 192, 1024)
    return pl.pallas_call(
        pair_kernel,
        in_specs=[VMEM, VMEM],
        out_specs=HBM,
        out_shape=jax.ShapeDtypeStruct(shape, bf16),
        scratch_shapes=[pltpu.VMEM(shape, bf16), pltpu.SemaphoreType.DMA((8,))],
        compiler_params=pltpu.CompilerParams(vmem_limit_bytes=24 * 2**20),
        name="pair_sum",
    )(own, got)


def fm_back_kernel(rank_ref, *refs):
    dns = refs[:4]
    recv_ref, projpad_ref, normed_ref, inv_ref, mix_ref = refs[4:9]
    sends = refs[9 : 9 + MP]
    block_ref, scr, rows = refs[9 + MP :]
    mask = flat_mask()
    inv = inv_ref[...][:, 0:1]
    dots = jnp.zeros((UB, 1), f32)
    for j in range(MP):
        at = slice(j * E, (j + 1) * E)
        d = dns[0][0:UB, at].astype(f32)
        for s in range(1, 4):
            d = d + dns[s][0:UB, at].astype(f32)
        scr[pl.ds(j, UB, stride=R), :] = d
        dots = dots + jnp.sum(d * normed_ref[:, at], axis=1, keepdims=True)
    mean = dots * (1.0 / (E * R))
    for j in range(MP):
        at = slice(j * E, (j + 1) * E)
        d = scr[pl.ds(j, UB, stride=R), :]
        scr[pl.ds(j, UB, stride=R), :] = inv * (d - normed_ref[:, at] * mean)
    projpad = projpad_ref[...]

    def step(u, carry):
        at = pl.multiple_of(u * R, R)
        p = user_rows(recv_ref, u)
        g = scr[pl.ds(at, R), :]
        spread = jnp.concatenate(
            [jnp.broadcast_to(g[j : j + 1, :], (FH, E)) for j in range(MP)], axis=0
        )
        spread = jnp.where(mask, spread, 0.0).astype(bf16)
        back = jnp.sum(dot(spread, p, TN).reshape(FH, R, E), axis=0)
        high = back.astype(bf16).astype(f32)
        pair = jnp.concatenate([high, back - high], axis=0).astype(bf16)
        back_rows = jnp.concatenate([pair] * 8, axis=0)
        left = jnp.concatenate([spread, projpad], axis=1)
        right = jnp.concatenate([tile_ranks(mix_ref[pl.ds(at, R), :]), back_rows], axis=0)
        grad = dot(left, right).astype(bf16)
        for j in range(MP):
            rows[j, pl.ds(pl.multiple_of(u * FH, FH), FH), :] = grad[j * FH : (j + 1) * FH, :]
        return carry

    lax.fori_loop(0, UB, step, 0, unroll=32)
    for s in range(MP):
        sends[s][...] = rows[rank_ref[0] ^ s]
    out = dns[0][UB : UB + 16, :].astype(f32)
    for s in range(1, 4):
        out = out + dns[s][UB : UB + 16, :].astype(f32)
    out = out.astype(bf16)
    for a in range(4):
        block_ref[a * 16 : (a + 1) * 16, :] = out[:, a * U : (a + 1) * U]


def fm_back_call(rank, dns, recv, projpad, normed, inv, mix):
    args = list(dns) + [recv, projpad, normed, inv, mix]
    whole = lambda shape: pl.BlockSpec(shape, lambda i, r: (0,) * len(shape))
    return pl.pallas_call(
        fm_back_kernel,
        grid_spec=pltpu.PrefetchScalarGridSpec(
            num_scalar_prefetch=1,
            grid=(1,),
            in_specs=[whole(x.shape) for x in args],
            out_specs=[whole((UB * FH, E))] * MP + [whole((64, U))],
            scratch_shapes=[pltpu.VMEM((UB * R, E), f32), pltpu.VMEM((MP, UB * FH, E), bf16)],
        ),
        out_shape=[jax.ShapeDtypeStruct((UB * FH, E), bf16)] * MP
        + [jax.ShapeDtypeStruct((64, U), bf16)],
        name="fm_backward",
    )(rank, *args)


def query_kernel(idx_ref, ev_ref, *refs):
    gps, (w_ref, out_ref, pooled_ref, scr, acc) = refs[:MP], refs[MP:]
    i = pl.program_id(0)
    mask = own_lanes()
    for s in range(MP):

        @pl.when(i == s)
        def _():
            pooled_ref[...] = gps[s][...]

    for u in range(UB):
        c = dot(pooled_ref[u * FH : (u + 1) * FH, :], ev_ref[u * E : (u + 1) * E, :], NT)
        scr[u : u + 1, :] = jnp.sum(jnp.where(mask, c, 0.0), axis=0, keepdims=True)
    w = w_ref[...]
    contrib = scr[...]
    d = w * (contrib - group_reduce(w * contrib, jnp.add))
    scr[...] = d
    parts = []
    for u in range(UB):
        row = jnp.broadcast_to(scr[u : u + 1, :], (FH, E))
        parts.append(jnp.where(mask, row, 0.0).astype(bf16))
    term = dot(jnp.concatenate(parts, axis=1), ev_ref[...])

    @pl.when(i == 0)
    def _():
        acc[...] = term

    @pl.when(i > 0)
    def _():
        acc[...] += term

    @pl.when(i == pl.num_programs(0) - 1)
    def _():
        out_ref[...] = acc[...] * (1.0 / math.sqrt(E))


def query_call(idx, ev, gps, w):
    return pl.pallas_call(
        query_kernel,
        grid_spec=pltpu.PrefetchScalarGridSpec(
            num_scalar_prefetch=1,
            grid=(MP,),
            in_specs=[pl.BlockSpec((UB * E, E), lambda i, t: (t[i], 0))]
            + [pl.BlockSpec((UB * FH, E), lambda i, t: (0, 0))] * MP
            + [pl.BlockSpec((UB, E), lambda i, t: (t[i], 0))],
            out_specs=[
                pl.BlockSpec((FH, E), lambda i, t: (0, 0)),
                pl.BlockSpec((UB * FH, E), lambda i, t: (t[i], 0)),
            ],
            scratch_shapes=[pltpu.VMEM((UB, E), f32), pltpu.VMEM((FH, E), f32)],
        ),
        out_shape=[
            jax.ShapeDtypeStruct((FH, E), f32),
            jax.ShapeDtypeStruct((U * FH, E), bf16),
        ],
        name="query_gradient",
    )(idx, ev, *gps, w)


CHUNK = (192, 1024)
HALVES = [jax.ShapeDtypeStruct((1024, 2048), f32), jax.ShapeDtypeStruct((2048, 512), f32)]


def half_kernel(half_ref, stack, *refs):
    up_hbm, down_hbm, up, down, up_sem, down_sem = refs[-6:]
    cols = pl.ds(pl.multiple_of(half_ref[0] * HALF, HALF), HALF)
    stores = []
    for i in range(8):
        at = i * E
        up[at : at + E, :] = stack[i, 0:E, :].astype(f32)
        down[at : at + 64, :] = stack[i, E:, 0:512].astype(f32)
        down[at + 64 : at + E, :] = stack[i, E:, 512:].astype(f32)
        rows = pl.ds(at, E)
        out_rows = pl.ds(pl.multiple_of(half_ref[0] * HALF + at, E), E)
        stores += [
            pltpu.make_async_copy(up.at[rows], up_hbm.at[rows, cols], up_sem.at[i]),
            pltpu.make_async_copy(down.at[rows], down_hbm.at[out_rows], down_sem.at[i]),
        ]
        start_all(stores[-2:])
    wait_all(stores)


def half_call(half, stack, outs=()):
    return pl.pallas_call(
        half_kernel,
        in_specs=[pl.BlockSpec(memory_space=pltpu.SMEM), VMEM] + [HBM] * len(outs),
        out_specs=[HBM, HBM],
        out_shape=HALVES,
        scratch_shapes=[pltpu.VMEM((1024, 1024), f32), pltpu.VMEM((1024, 512), f32)]
        + [pltpu.SemaphoreType.DMA((8,))] * 2,
        input_output_aliases={2: 0, 3: 1} if outs else {},
        compiler_params=pltpu.CompilerParams(vmem_limit_bytes=24 * 2**20),
        name="other_half" if outs else "own_half",
    )(half, stack, *outs)


SAME_CORE = [[2 * i + c for i in range(8)] for c in range(2)]


def dp_exchange(x):
    return lax.all_to_all(x, "dp", 0, 0, axis_index_groups=SAME_CORE, tiled=True)


def core_swap(x):
    return lax.ppermute(x, "dp", [(i, i ^ 1) for i in range(16)])


def mp_permute(x, s):
    return lax.ppermute(x, "mp", [(i, i ^ s) for i in range(MP)])


def exchange_slots(xs):
    got = [xs[0]]
    for s in range(1, MP):
        got.append(mp_permute(xs[s], s))
    return got


def dp_permute(x, s):
    pairs = [
        (h * 8 + z * 2 + c, (h ^ (s // 4)) * 8 + ((z + s) % 4) * 2 + c)
        for h in range(2)
        for z in range(4)
        for c in range(2)
    ]
    return lax.ppermute(x, "dp", pairs)


def exchange(x):
    return lax.all_to_all(x, "mp", 0, 0, tiled=True)


def device_step(events, lengths, query_vecs, fm_proj, up_weight, down_weight, cotangent):
    c = lax.axis_index("dp") % 2
    m = lax.axis_index("mp")
    ev = events.reshape(U * FH * L, E)
    send, weights = pool_call(ev, lengths.T, query_vecs, cotangent.T)
    recv = exchange(send)
    projt = jnp.pad(fm_proj.T, ((0, 8), (0, 0)))
    projpad = jnp.pad(jnp.concatenate([fm_proj, fm_proj], axis=1), ((0, 0), (0, E - 2 * R)))
    rows, normed, inv, mix, cot_full = fm_call(recv, projt)
    n = exchange(rows).reshape(U, E * R)

    other = (1 - c)[None].astype(jnp.int32)
    mine = c[None].astype(jnp.int32)
    rank = m[None].astype(jnp.int32)
    slots = (m ^ jnp.arange(MP)).astype(jnp.int32)
    layer = (rank, n, cot_full, up_weight, down_weight)
    g_other, *others = layer_call(other, *layer)
    got = core_swap(g_other)
    g_mine, cross, keep = layer_call(mine, *layer, tuple(others))
    crossed = mp_permute(cross, 1)
    pair = pair_call(g_mine, got)
    parts = dp_exchange(pair)

    dns = [(keep[k].astype(f32) + crossed[k].astype(f32)).astype(bf16) for k in range(4)]
    dns = dns[:1] + [mp_permute(dns[k], 2 * k) for k in range(1, 4)]
    *gp_sends, block_out = fm_back_call(rank, dns, recv, projpad, normed, inv, mix)

    chunk = jnp.sum(parts.astype(f32), axis=0).astype(bf16)
    stack = dp_exchange(jnp.broadcast_to(chunk[None], (8,) + CHUNK))

    gps = exchange_slots(gp_sends)
    query_term, grad_pooled = query_call(slots, ev, gps, weights)
    grad_pooled = grad_pooled.reshape(U, FH, E)
    query_other = core_swap(query_term)
    query_pair = (query_term + query_other).astype(bf16)
    query_parts = [query_pair] + [dp_permute(query_pair, s) for s in range(1, 8)]
    grad_query = sum(x.astype(f32) for x in query_parts)

    stack_other = core_swap(stack)
    halves = half_call(mine, stack)
    grad_up, grad_down = half_call(other, stack_other, halves)
    return (block_out.T, grad_up, grad_down, grad_pooled, grad_query)


def solution(mesh):
    in_specs = (
        P("dp", "mp", None, None),
        P("dp", "mp"),
        P("mp", None),
        P(),
        P(None, "mp"),
        P("mp", None),
        P("dp", "mp"),
    )
    out_specs = (P("dp", "mp"), P(None, "mp"), P("mp", None), P("dp", "mp", None), P("mp", None))
    return jax.shard_map(
        device_step, mesh=mesh, in_specs=in_specs, out_specs=out_specs, check_vma=False
    )
```

```python
import math

import jax
import jax.numpy as jnp
from jax import lax
from jax.experimental import pallas as pl
from jax.experimental.pallas import tpu as pltpu
from jax.sharding import PartitionSpec as P


norm_eps = 1e-05
f32 = jnp.float32
bf16 = jnp.bfloat16


E = 128
L = 8
R = 8
MP = 8
FH = 16
UB = 32
U = 256
NT = (((1,), (1,)), ((), ()))
TN = (((0,), (0,)), ((), ()))
NN = (((1,), (0,)), ((), ()))


def dot(a, b, dims=NN):
    return lax.dot_general(a, b, dims, preferred_element_type=f32)


def iota(shape, axis):
    return lax.broadcasted_iota(jnp.int32, shape, axis)


def own_lanes():
    return iota((FH, E), 0) == iota((FH, E), 1) // L


def group_reduce(x, op):
    lane = iota(x.shape, 1)
    for s in (1, 2, 4):
        up = pltpu.roll(x, E - s, 1)
        down = pltpu.roll(x, s, 1)
        x = op(x, jnp.where((lane & s) == 0, up, down))
    return x


PARTS = 2
PER = MP // PARTS


def pool_kernel(
    ev_hbm, lent_ref, q_ref, cott_ref, send_hbm, w_hbm, ev, send, w, in_sem, out_sem, w_sem
):
    rows = PER * UB * E
    loads = [
        pltpu.make_async_copy(ev_hbm.at[pl.ds(g * rows, rows)], ev.at[g], in_sem.at[g])
        for g in range(PARTS)
    ]
    for load in loads:
        load.start()
    mask = own_lanes()
    spread = mask.astype(f32).astype(bf16)
    lens = dot(lent_ref[...].astype(f32).astype(bf16), spread, TN)
    live = (iota((U, E), 1) % L).astype(f32) < lens
    q = q_ref[...]
    copies = []
    for g in range(PARTS):
        loads[g].wait()
        raw = dot(q, ev[g], NT)
        first = g * PER * UB
        here = slice(first, first + PER * UB)
        for u in range(PER * UB):
            block = jnp.where(mask, raw[:, u * E : (u + 1) * E], 0.0)
            w[first + u : first + u + 1, :] = jnp.sum(block, axis=0, keepdims=True)
        scores = w[here, :] * (1.0 / math.sqrt(E))
        top = group_reduce(jnp.where(live[here], scores, -1e30), jnp.maximum)
        ex = jnp.exp(jnp.where(live[here], scores - top, -1e30))
        w[here, :] = ex / group_reduce(ex, jnp.add)
        for i in range(PER):
            p = g * PER + i
            for u in range(UB):
                row = jnp.broadcast_to(w[p * UB + u : p * UB + u + 1, :], (FH, E))
                weight = jnp.where(mask, row, 0.0).astype(bf16)
                at = (i * UB + u) * E
                pooled = dot(weight, ev[g, at : at + E, :])
                send[p, u * FH : (u + 1) * FH, :] = pooled.astype(bf16)
            send[p, UB * FH : UB * FH + 64, :] = cott_ref[:, 0:E]
            send[p, UB * FH + 64 :, :] = cott_ref[:, E:]
            copies.append(pltpu.make_async_copy(send.at[p], send_hbm.at[p], out_sem.at[p]))
            copies[-1].start()
    copies.append(pltpu.make_async_copy(w, w_hbm, w_sem))
    copies[-1].start()
    wait_all(copies)


HBM = pl.BlockSpec(memory_space=pltpu.HBM)
VMEM = pl.BlockSpec(memory_space=pltpu.VMEM)


def pool_call(ev, lent, q, cott):
    rows = UB * FH + U // 2
    return pl.pallas_call(
        pool_kernel,
        in_specs=[HBM, VMEM, VMEM, VMEM],
        out_specs=[HBM, HBM],
        out_shape=[
            jax.ShapeDtypeStruct((MP, rows, E), bf16),
            jax.ShapeDtypeStruct((U, E), f32),
        ],
        scratch_shapes=[
            pltpu.VMEM((PARTS, PER * UB * E, E), bf16),
            pltpu.VMEM((MP, rows, E), bf16),
            pltpu.VMEM((U, E), f32),
            pltpu.SemaphoreType.DMA((PARTS,)),
            pltpu.SemaphoreType.DMA((MP,)),
            pltpu.SemaphoreType.DMA,
        ],
        name="pool",
    )(ev, lent, q, cott)


def flat_mask():
    return iota((E, E), 0) % FH == iota((E, E), 1) // R


def tile_ranks(m):
    pair = jnp.concatenate([m, m], axis=0).astype(bf16)
    return jnp.concatenate([pair] * 8, axis=0)


def user_rows(ref, u):
    return jnp.concatenate(
        [ref[j, pl.ds(pl.multiple_of(u * FH, FH), FH), :] for j in range(MP)], axis=0
    )


def fm_kernel(recv_ref, projt_ref, *refs):
    outs, (rows, normed, inv_v, mix_v, cot, scr, row_sem, sem) = refs[:5], refs[5:]
    mask = flat_mask()
    projt = projt_ref[...]
    at = UB * FH
    for j in range(MP):
        cot[j * 64 : (j + 1) * 64, 0:E] = recv_ref[j, at : at + 64, :]
        cot[j * 64 : (j + 1) * 64, E:] = recv_ref[j, at + 64 :, :]
    copies = [
        pltpu.make_async_copy(v, o, sem.at[i])
        for i, (v, o) in enumerate(zip((normed, inv_v, mix_v, cot), outs[1:]))
    ]
    copies[3].start()

    def step(u, carry):
        p = user_rows(recv_ref, u)
        mix = dot(projt, p)[0:R].astype(bf16).astype(f32)
        full = jnp.where(mask, dot(p, tile_ranks(mix), NT), 0.0)
        at = pl.multiple_of(u * R, R)
        mix_v[pl.ds(at, R), :] = mix
        scr[pl.ds(at, R), :] = jnp.sum(full.reshape(MP, FH, E), axis=1)
        return carry

    lax.fori_loop(0, UB, step, 0, unroll=32)
    copies[2].start()
    total = jnp.zeros((UB, 1), f32)
    for j in range(MP):
        x = scr[pl.ds(j, UB, stride=R), :]
        total = total + jnp.sum(x * x, axis=1, keepdims=True)
    inv = lax.rsqrt(total * (1.0 / (E * R)) + norm_eps)
    inv_v[...] = jnp.broadcast_to(inv, (UB, E))
    for j in range(MP):
        x = scr[pl.ds(j, UB, stride=R), :] * inv
        normed[:, j * E : (j + 1) * E] = x
        rows[:, j * E : (j + 1) * E] = x.astype(bf16)
    copies += [pltpu.make_async_copy(rows, outs[0].at[p], row_sem.at[p]) for p in range(MP)]
    start_all(copies[4:])
    start_all(copies[:2])
    wait_all(copies)


def fm_call(recv, projt):
    return pl.pallas_call(
        fm_kernel,
        in_specs=[VMEM, VMEM],
        out_specs=[HBM] * 5,
        out_shape=[
            jax.ShapeDtypeStruct((MP, UB, E * R), bf16),
            jax.ShapeDtypeStruct((UB, E * R), f32),
            jax.ShapeDtypeStruct((UB, E), f32),
            jax.ShapeDtypeStruct((UB * R, E), f32),
            jax.ShapeDtypeStruct((512, U), bf16),
        ],
        scratch_shapes=[
            pltpu.VMEM((UB, E * R), bf16),
            pltpu.VMEM((UB, E * R), f32),
            pltpu.VMEM((UB, E), f32),
            pltpu.VMEM((UB * R, E), f32),
            pltpu.VMEM((512, U), bf16),
            pltpu.VMEM((UB * R, E), f32),
            pltpu.SemaphoreType.DMA((MP,)),
            pltpu.SemaphoreType.DMA((4,)),
        ],
        name="fm_forward",
    )(recv, projt)


HB = 256
STEPS = 4
FIRST_KIB, SECOND_KIB = 28000, 28000
HALF = HB * STEPS


def turn_kernel(cott, up, down, cot):
    cot[...] = cott[...].T


def turn_call(cott, up, down):
    return pl.pallas_call(
        turn_kernel,
        in_specs=[VMEM] * 3,
        out_specs=VMEM,
        out_shape=jax.ShapeDtypeStruct((U, 512), bf16),
        compiler_params=pltpu.CompilerParams(vmem_limit_bytes=FIRST_KIB * 1024),
        name="turn",
    )(cott, up, down)


def start_all(copies):
    for copy in copies:
        copy.start()


def wait_all(copies):
    for copy in copies:
        copy.wait()


def layer_half(half, n, nt, cot, up, down, act, dh, g):
    def block(k, carry):
        cols = pl.ds(pl.multiple_of(k * HB, HB), HB)
        units = pl.ds(pl.multiple_of(half * HALF + k * HB, HB), HB)
        hidden = dot(n[...], up[:, units])
        d_act = dot(cot[...], down[units, :], NT)
        s = 1.0 / (1.0 + jnp.exp(-hidden))
        act_k = (hidden * s).astype(bf16)
        dh_k = (d_act * s * (1.0 + hidden * (1.0 - s))).astype(bf16)
        act[:, cols] = act_k
        dh[:, cols] = dh_k
        g[:, 0:E, cols] = dot(nt[...], dh_k).astype(bf16).reshape(MP, E, HB)
        g_down = dot(act_k, cot[...], TN).astype(bf16)
        for t in range(2):
            for h in range(2):
                at = t * 128 + h * 64
                g[2 * k + t, E:, h * 512 : (h + 1) * 512] = g_down[at : at + 64, :]
        return carry

    lax.fori_loop(0, STEPS, block, 0)


def layer_first(half_ref, rank_ref, n, cot, up, down, g, act, dh, nt):
    nt[...] = n[...].T
    layer_half(half_ref[0], n, nt, cot, up, down, act, dh, g)


def layer_second(
    half_ref, rank_ref, n, cot, up, down, act_o, dh_o, g, cross, keep,
    nt, act, dh, dn, packed,
):
    half = half_ref[0]
    nt[...] = n[...].T
    layer_half(half, n, nt, cot, up, down, act, dh, g)
    units = [pl.ds(pl.multiple_of(h * HALF, HALF), HALF) for h in (half, 1 - half)]
    out = dot(act[...], down[units[0], :]) + dot(act_o[...], down[units[1], :])
    out = out.T
    for p in range(MP):
        for a in range(4):
            at = p * 64 + a * 16
            packed[p, :, a * U : (a + 1) * U] = out[at : at + 16, :].astype(bf16)
    dn[...] = dot(dh[...], up[:, units[0]], NT) + dot(dh_o[...], up[:, units[1]], NT)
    for k in range(4):
        for flip, to in ((1, cross), (0, keep)):
            p = rank_ref[0] ^ flip ^ (2 * k)
            to[k, 0:UB, :] = dn[pl.ds(pl.multiple_of(p * UB, UB), UB), :].astype(bf16)
            to[k, UB:, :] = packed[p]


def layer_call(half, rank, n, cot, up, down, others=()):
    slab = pltpu.VMEM((U, HALF), bf16)
    scratch = [pltpu.VMEM((E * R, U), bf16)]
    g_shape = jax.ShapeDtypeStruct((MP, 192, 1024), bf16)
    if others:
        body = layer_second
        scratch += [slab, slab, pltpu.VMEM((U, E * R), f32), pltpu.VMEM((MP, 16, 1024), bf16)]
        out_shape = [g_shape] + [jax.ShapeDtypeStruct((4, 48, 1024), bf16)] * 2
    else:
        body = layer_first
        out_shape = [g_shape] + [jax.ShapeDtypeStruct((U, HALF), bf16)] * 2
    return pl.pallas_call(
        body,
        in_specs=[pl.BlockSpec(memory_space=pltpu.SMEM)] * 2 + [VMEM] * (4 + len(others)),
        out_specs=[VMEM] * 3,
        out_shape=out_shape,
        scratch_shapes=scratch,
        compiler_params=pltpu.CompilerParams(
            vmem_limit_bytes=(SECOND_KIB if others else FIRST_KIB) * 1024
        ),
        name="layer_second" if others else "layer_first",
    )(half, rank, n, cot, up, down, *others)


def pair_kernel(own, got, out_hbm, total, sem):
    stores = [pltpu.make_async_copy(total.at[t], out_hbm.at[t], sem.at[t]) for t in range(8)]
    for t in range(8):
        total[t] = (own[t].astype(f32) + got[t].astype(f32)).astype(bf16)
        stores[t].start()
    wait_all(stores)


def pair_call(own, got):
    shape = (8, 192, 1024)
    return pl.pallas_call(
        pair_kernel,
        in_specs=[VMEM, VMEM],
        out_specs=HBM,
        out_shape=jax.ShapeDtypeStruct(shape, bf16),
        scratch_shapes=[pltpu.VMEM(shape, bf16), pltpu.SemaphoreType.DMA((8,))],
        compiler_params=pltpu.CompilerParams(vmem_limit_bytes=24 * 2**20),
        name="pair_sum",
    )(own, got)


def fm_back_kernel(rank_ref, *refs):
    dns = refs[:4]
    recv_ref, projpad_ref, normed_ref, inv_ref, mix_ref = refs[4:9]
    sends = refs[9 : 9 + MP]
    block_ref, scr, rows = refs[9 + MP :]
    mask = flat_mask()
    inv = inv_ref[...][:, 0:1]
    dots = jnp.zeros((UB, 1), f32)
    for j in range(MP):
        at = slice(j * E, (j + 1) * E)
        d = dns[0][0:UB, at].astype(f32)
        for s in range(1, 4):
            d = d + dns[s][0:UB, at].astype(f32)
        scr[pl.ds(j, UB, stride=R), :] = d
        dots = dots + jnp.sum(d * normed_ref[:, at], axis=1, keepdims=True)
    mean = dots * (1.0 / (E * R))
    for j in range(MP):
        at = slice(j * E, (j + 1) * E)
        d = scr[pl.ds(j, UB, stride=R), :]
        scr[pl.ds(j, UB, stride=R), :] = inv * (d - normed_ref[:, at] * mean)
    projpad = projpad_ref[...]

    def step(u, carry):
        at = pl.multiple_of(u * R, R)
        p = user_rows(recv_ref, u)
        g = scr[pl.ds(at, R), :]
        spread = jnp.concatenate(
            [jnp.broadcast_to(g[j : j + 1, :], (FH, E)) for j in range(MP)], axis=0
        )
        spread = jnp.where(mask, spread, 0.0).astype(bf16)
        back = jnp.sum(dot(spread, p, TN).reshape(FH, R, E), axis=0)
        high = back.astype(bf16).astype(f32)
        pair = jnp.concatenate([high, back - high], axis=0).astype(bf16)
        back_rows = jnp.concatenate([pair] * 8, axis=0)
        left = jnp.concatenate([spread, projpad], axis=1)
        right = jnp.concatenate([tile_ranks(mix_ref[pl.ds(at, R), :]), back_rows], axis=0)
        grad = dot(left, right).astype(bf16)
        for j in range(MP):
            rows[j, pl.ds(pl.multiple_of(u * FH, FH), FH), :] = grad[j * FH : (j + 1) * FH, :]
        return carry

    lax.fori_loop(0, UB, step, 0, unroll=32)
    for s in range(MP):
        sends[s][...] = rows[rank_ref[0] ^ s]
    out = dns[0][UB : UB + 16, :].astype(f32)
    for s in range(1, 4):
        out = out + dns[s][UB : UB + 16, :].astype(f32)
    out = out.astype(bf16)
    for a in range(4):
        block_ref[a * 16 : (a + 1) * 16, :] = out[:, a * U : (a + 1) * U]


def fm_back_call(rank, dns, recv, projpad, normed, inv, mix):
    args = list(dns) + [recv, projpad, normed, inv, mix]
    whole = lambda shape: pl.BlockSpec(shape, lambda i, r: (0,) * len(shape))
    return pl.pallas_call(
        fm_back_kernel,
        grid_spec=pltpu.PrefetchScalarGridSpec(
            num_scalar_prefetch=1,
            grid=(1,),
            in_specs=[whole(x.shape) for x in args],
            out_specs=[whole((UB * FH, E))] * MP + [whole((64, U))],
            scratch_shapes=[pltpu.VMEM((UB * R, E), f32), pltpu.VMEM((MP, UB * FH, E), bf16)],
        ),
        out_shape=[jax.ShapeDtypeStruct((UB * FH, E), bf16)] * MP
        + [jax.ShapeDtypeStruct((64, U), bf16)],
        compiler_params=pltpu.CompilerParams(vmem_limit_bytes=52 * 2**20),
        name="fm_backward",
    )(rank, *args)


def query_kernel(idx_ref, ev_ref, *refs):
    gps, (w_ref, out_ref, pooled_ref, scr, acc) = refs[:MP], refs[MP:]
    i = pl.program_id(0)
    mask = own_lanes()
    for s in range(MP):

        @pl.when(i == s)
        def _():
            pooled_ref[...] = gps[s][...]

    for u in range(UB):
        c = dot(pooled_ref[u * FH : (u + 1) * FH, :], ev_ref[u * E : (u + 1) * E, :], NT)
        scr[u : u + 1, :] = jnp.sum(jnp.where(mask, c, 0.0), axis=0, keepdims=True)
    w = w_ref[...]
    contrib = scr[...]
    d = w * (contrib - group_reduce(w * contrib, jnp.add))
    scr[...] = d
    parts = []
    for u in range(UB):
        row = jnp.broadcast_to(scr[u : u + 1, :], (FH, E))
        parts.append(jnp.where(mask, row, 0.0).astype(bf16))
    term = dot(jnp.concatenate(parts, axis=1), ev_ref[...])

    @pl.when(i == 0)
    def _():
        acc[...] = term

    @pl.when(i > 0)
    def _():
        acc[...] += term

    @pl.when(i == pl.num_programs(0) - 1)
    def _():
        out_ref[...] = acc[...] * (1.0 / math.sqrt(E))


def query_call(idx, ev, gps, w):
    return pl.pallas_call(
        query_kernel,
        grid_spec=pltpu.PrefetchScalarGridSpec(
            num_scalar_prefetch=1,
            grid=(MP,),
            in_specs=[pl.BlockSpec((UB * E, E), lambda i, t: (t[i], 0))]
            + [pl.BlockSpec((UB * FH, E), lambda i, t: (0, 0))] * MP
            + [pl.BlockSpec((UB, E), lambda i, t: (t[i], 0))],
            out_specs=[
                pl.BlockSpec((FH, E), lambda i, t: (0, 0)),
                pl.BlockSpec((UB * FH, E), lambda i, t: (t[i], 0)),
            ],
            scratch_shapes=[pltpu.VMEM((UB, E), f32), pltpu.VMEM((FH, E), f32)],
        ),
        out_shape=[
            jax.ShapeDtypeStruct((FH, E), f32),
            jax.ShapeDtypeStruct((U * FH, E), bf16),
        ],
        name="query_gradient",
    )(idx, ev, *gps, w)


CHUNK = (192, 1024)
HALVES = [jax.ShapeDtypeStruct((1024, 2048), f32), jax.ShapeDtypeStruct((2048, 512), f32)]


def half_kernel(half_ref, stack, *refs):
    up_hbm, down_hbm, up, down, up_sem, down_sem = refs[-6:]
    cols = pl.ds(pl.multiple_of(half_ref[0] * HALF, HALF), HALF)
    stores = []
    for i in range(8):
        at = i * E
        up[at : at + E, :] = stack[i, 0:E, :].astype(f32)
        down[at : at + 64, :] = stack[i, E:, 0:512].astype(f32)
        down[at + 64 : at + E, :] = stack[i, E:, 512:].astype(f32)
        rows = pl.ds(at, E)
        out_rows = pl.ds(pl.multiple_of(half_ref[0] * HALF + at, E), E)
        stores += [
            pltpu.make_async_copy(up.at[rows], up_hbm.at[rows, cols], up_sem.at[i]),
            pltpu.make_async_copy(down.at[rows], down_hbm.at[out_rows], down_sem.at[i]),
        ]
        start_all(stores[-2:])
    wait_all(stores)


def half_call(half, stack, outs=()):
    return pl.pallas_call(
        half_kernel,
        in_specs=[pl.BlockSpec(memory_space=pltpu.SMEM), VMEM] + [HBM] * len(outs),
        out_specs=[HBM, HBM],
        out_shape=HALVES,
        scratch_shapes=[pltpu.VMEM((1024, 1024), f32), pltpu.VMEM((1024, 512), f32)]
        + [pltpu.SemaphoreType.DMA((8,))] * 2,
        input_output_aliases={2: 0, 3: 1} if outs else {},
        compiler_params=pltpu.CompilerParams(vmem_limit_bytes=24 * 2**20),
        name="other_half" if outs else "own_half",
    )(half, stack, *outs)


SAME_CORE = [[2 * i + c for i in range(8)] for c in range(2)]


def dp_exchange(x):
    return lax.all_to_all(x, "dp", 0, 0, axis_index_groups=SAME_CORE, tiled=True)


def core_swap(x):
    return lax.ppermute(x, "dp", [(i, i ^ 1) for i in range(16)])


def mp_permute(x, s):
    return lax.ppermute(x, "mp", [(i, i ^ s) for i in range(MP)])


def exchange_slots(xs):
    got = [xs[0]]
    for s in range(1, MP):
        got.append(mp_permute(xs[s], s))
    return got


def dp_permute(x, s):
    pairs = [
        (h * 8 + z * 2 + c, (h ^ (s // 4)) * 8 + ((z + s) % 4) * 2 + c)
        for h in range(2)
        for z in range(4)
        for c in range(2)
    ]
    return lax.ppermute(x, "dp", pairs)


def exchange(x):
    return lax.all_to_all(x, "mp", 0, 0, tiled=True)


def device_step(events, lengths, query_vecs, fm_proj, up_weight, down_weight, cotangent):
    c = lax.axis_index("dp") % 2
    m = lax.axis_index("mp")
    ev = events.reshape(U * FH * L, E)
    send, weights = pool_call(ev, lengths.T, query_vecs, cotangent.T)
    recv = exchange(send)
    projt = jnp.pad(fm_proj.T, ((0, 8), (0, 0)))
    projpad = jnp.pad(jnp.concatenate([fm_proj, fm_proj], axis=1), ((0, 0), (0, E - 2 * R)))
    rows, normed, inv, mix, cot_full = fm_call(recv, projt)
    n = exchange(rows).reshape(U, E * R)
    cot = turn_call(cot_full, up_weight, down_weight)

    other = (1 - c)[None].astype(jnp.int32)
    mine = c[None].astype(jnp.int32)
    rank = m[None].astype(jnp.int32)
    slots = (m ^ jnp.arange(MP)).astype(jnp.int32)
    layer = (rank, n, cot, up_weight, down_weight)
    g_other, *others = layer_call(other, *layer)
    got = core_swap(g_other)
    g_mine, cross, keep = layer_call(mine, *layer, tuple(others))
    crossed = mp_permute(cross, 1)
    pair = pair_call(g_mine, got)
    parts = dp_exchange(pair)

    dns = [(keep[k].astype(f32) + crossed[k].astype(f32)).astype(bf16) for k in range(4)]
    dns = dns[:1] + [mp_permute(dns[k], 2 * k) for k in range(1, 4)]
    *gp_sends, block_out = fm_back_call(rank, dns, recv, projpad, normed, inv, mix)

    chunk = jnp.sum(parts.astype(f32), axis=0).astype(bf16)
    stack = dp_exchange(jnp.broadcast_to(chunk[None], (8,) + CHUNK))

    gps = exchange_slots(gp_sends)
    query_term, grad_pooled = query_call(slots, ev, gps, weights)
    grad_pooled = grad_pooled.reshape(U, FH, E)
    query_other = core_swap(query_term)
    query_pair = (query_term + query_other).astype(bf16)
    query_parts = [query_pair] + [dp_permute(query_pair, s) for s in range(1, 8)]
    grad_query = sum(x.astype(f32) for x in query_parts)

    stack_other = core_swap(stack)
    halves = half_call(mine, stack)
    grad_up, grad_down = half_call(other, stack_other, halves)
    return (block_out.T, grad_up, grad_down, grad_pooled, grad_query)


def solution(mesh):
    in_specs = (
        P("dp", "mp", None, None),
        P("dp", "mp"),
        P("mp", None),
        P(),
        P(None, "mp"),
        P("mp", None),
        P("dp", "mp"),
    )
    out_specs = (P("dp", "mp"), P(None, "mp"), P("mp", None), P("dp", "mp", None), P("mp", None))
    return jax.shard_map(
        device_step, mesh=mesh, in_specs=in_specs, out_specs=out_specs, check_vma=False
    )
```
